32 devices in a mesh: img: 4 (over y, x), seq: 8 (over z, core).
Axes of the slice: x: 2, y: 2, z: 4, core: 2. Of those that a mesh axis runs over, the one named last changes fastest.
Arguments:
- image_query: bfloat16 [4, 1024, 1280], P('img', 'seq'), may hold values from -7 to 7
- image_key: bfloat16 [4, 1024, 1280], P('img', 'seq'), may hold values from -7 to 7
- image_value: bfloat16 [4, 1024, 1280], P('img', 'seq'), may hold values from -3 to 3
- image_output: bfloat16 [4, 1024, 1280], P('img', 'seq'), may hold values from -0.875 to 0.875
- output_grad: bfloat16 [4, 1024, 2432], P('img', 'seq'), may hold values from -48 to 48
- image_logsum: float32 [4, 1024, 20], P('img', 'seq'), may hold values from 8 to 9
- text_query: bfloat16 [4, 333, 1280], P('img'), may hold values from -7 to 7
- text_key: bfloat16 [4, 333, 1280], P('img'), may hold values from -7 to 7
- text_value: bfloat16 [4, 333, 1280], P('img'), may hold values from -3 to 3
- text_output: bfloat16 [4, 333, 1280], P('img'), may hold values from -0.875 to 0.875
- text_grad: bfloat16 [4, 333, 1280], P('img'), may hold values from -48 to 48
- text_logsum: float32 [4, 333, 20], P('img'), may hold values from 8 to 9
- out_weight: bfloat16 [2432, 1280], replicated, may hold values from -0.125 to 0.125
Outputs:
- query_grad: bfloat16 [4, 1024, 1280], P('img', 'seq')
- key_grad: bfloat16 [4, 1024, 1280], P('img', 'seq')
- value_grad: bfloat16 [4, 1024, 1280], P('img', 'seq')
- text_query_grad: bfloat16 [4, 333, 1280], P('img')
- text_key_grad: bfloat16 [4, 333, 1280], P('img')
- text_value_grad: bfloat16 [4, 333, 1280], P('img')
- weight_grad: float32 [2432, 1280], P('seq')
The draws below stay inside these ranges and needn't reach their ends.
All inputs are finite; a program needn't handle non-finite values.
Results may differ from the reference program's by a relative error of at most 0.017.
Values may be sent and summed in bfloat16 or wider, within the bound.
A program may use at most 192 MiB of HBM per device.

```python
import jax
import jax.numpy as jnp
from jax import lax

D = 2432
HEADS = 20
TXT = 333
TOK_DEV = 128
HD = 1280
S = 1024
IMAGES = 4
N_SEQ = 8


def levels(key, extent, cuts, low, largest):
    factor_of, own = 1.0, jax.random.fold_in(key, 6)
    for axis_at, parts in cuts:
        steps = jnp.exp(jax.random.uniform(jax.random.fold_in(own, axis_at), (parts,), jnp.float32, low / len(cuts), largest / len(cuts)))
        factor_of = factor_of * jnp.repeat(steps, extent[axis_at] // parts).reshape([-1 if axis == axis_at else 1 for axis in range(len(extent))])
    return factor_of


def centred(own_key, shape, spread, limit, split=(), dtype=jnp.bfloat16):
    result = jax.random.normal(own_key, shape, jnp.float32) * spread
    if len(split) > 0:
        result = levels(own_key, shape, split, -0.22, 0.18) * result
    return jnp.clip(result, min=-limit, max=limit).astype(dtype)


def setup_inputs(seed: int = 0) -> dict:
    keys = jax.random.split(jax.random.key(seed), 14)
    return {
        "image_query": centred(keys[0], (IMAGES, S, HD), 1.1, 7.0, ((0, 4), (1, 8))),
        "image_key": centred(keys[1], (IMAGES, S, HD), 1.1, 7.0, ((0, 4), (1, 8))),
        "image_value": centred(keys[2], (IMAGES, S, HD), 0.5, 3.0, ((0, 4), (1, 8))),
        "image_output": centred(keys[3], (IMAGES, S, HD), 0.15, 0.875, ((0, 4), (1, 8))),
        "output_grad": centred(keys[4], (IMAGES, S, D), 8.0, 48.0, ((0, 4), (1, 8))),
        "image_logsum": jnp.clip(8.0 + 1.0 * jax.random.uniform(keys[5], (IMAGES, S, HEADS), jnp.float32) ** levels(keys[5], (IMAGES, S, HEADS), ((0, 4), (1, 8)), -0.2, 0.2), 8.0, 9.0),
        "text_query": centred(keys[6], (IMAGES, TXT, HD), 1.1, 7.0, ((0, 4),)),
        "text_key": centred(keys[7], (IMAGES, TXT, HD), 1.1, 7.0, ((0, 4),)),
        "text_value": centred(keys[8], (IMAGES, TXT, HD), 0.5, 3.0, ((0, 4),)),
        "text_output": centred(keys[9], (IMAGES, TXT, HD), 0.15, 0.875, ((0, 4),)),
        "text_grad": centred(keys[10], (IMAGES, TXT, HD), 8.0, 48.0, ((0, 4),)),
        "text_logsum": jnp.clip(8.0 + 1.0 * jax.random.uniform(keys[11], (IMAGES, TXT, HEADS), jnp.float32) ** levels(keys[11], (IMAGES, TXT, HEADS), ((0, 4),), -0.2, 0.2), 8.0, 9.0),
        "out_weight": centred(keys[12], (D, HD), D ** -0.5, 0.125),
    }


def row_dot(grads_out, outputs, head_count):
    product = grads_out.astype(jnp.float32) * outputs.astype(jnp.float32)
    return product.reshape(product.shape[0], head_count, -1).sum(axis=-1)


def pair_grads(queries, grads_out, log_sum, row_dots, key_rows, value_rows):
    head_count = log_sum.shape[1]
    query_count = queries.shape[0]
    key_count = key_rows.shape[0]
    head_width = queries.shape[1] // head_count
    scaling = head_width ** -0.5
    query_heads = queries.astype(jnp.float32).reshape(query_count, head_count, head_width)
    grad_heads = grads_out.astype(jnp.float32).reshape(query_count, head_count, head_width)
    key_heads = key_rows.astype(jnp.float32).reshape(key_count, head_count, head_width)
    value_heads = value_rows.astype(jnp.float32).reshape(key_count, head_count, head_width)
    scores = jnp.einsum("qhe,khe->hqk", query_heads, key_heads) * scaling
    weights = jnp.exp(scores - log_sum.T[:, :, None])
    grad_weights = jnp.einsum("qhe,khe->hqk", grad_heads, value_heads)
    grad_scores = weights * (grad_weights - row_dots.T[:, :, None])
    weights_low = lax.optimization_barrier(weights.astype(jnp.bfloat16)).astype(jnp.float32)
    scores_low = lax.optimization_barrier(grad_scores.astype(jnp.bfloat16)).astype(jnp.float32)
    query_part = jnp.einsum("hqk,khe->qhe", scores_low, key_heads) * scaling
    key_part = jnp.einsum("hqk,qhe->khe", scores_low, query_heads) * scaling
    value_part = jnp.einsum("hqk,qhe->khe", weights_low, grad_heads)
    return (query_part.reshape(query_count, -1), key_part.reshape(key_count, -1),
            value_part.reshape(key_count, -1))


def reference(image_query, image_key, image_value, image_output, output_grad, image_logsum,
              text_query, text_key, text_value, text_output, text_grad, text_logsum, out_weight):
    head_count = image_logsum.shape[-1]

    def one_image(inputs):
        (queries, key_rows, value_rows, outputs, upstream, log_sum,
         text_queries, text_keys, text_values, text_outs, text_dout, text_lsum) = inputs
        image_dout = jnp.dot(upstream, out_weight, preferred_element_type=jnp.float32).astype(jnp.bfloat16)
        image_dots = row_dot(image_dout, outputs, head_count)
        text_dots = row_dot(text_dout, text_outs, head_count)
        all_keys = jnp.concatenate([key_rows, text_keys], axis=0)
        all_values = jnp.concatenate([value_rows, text_values], axis=0)
        feature = queries.shape[1]
        length = queries.shape[0]

        def query_block(running, section):
            block_query, block_dout, block_lsum, block_dots = section
            query_part, key_part, value_part = pair_grads(block_query, block_dout, block_lsum, block_dots,
                                                          all_keys, all_values)
            return (running[0] + key_part, running[1] + value_part), query_part

        zeros_grad = jnp.zeros(all_keys.shape, jnp.float32)
        sections = (queries.reshape(N_SEQ, TOK_DEV, feature), image_dout.reshape(N_SEQ, TOK_DEV, feature),
                    log_sum.reshape(N_SEQ, TOK_DEV, head_count), image_dots.reshape(N_SEQ, TOK_DEV, head_count))
        (key_total, value_total), query_blocks = lax.scan(query_block, (zeros_grad, zeros_grad), sections)
        text_qpart, text_kpart, text_vpart = pair_grads(text_queries, text_dout, text_lsum, text_dots,
                                                        all_keys, all_values)
        key_total = key_total + text_kpart
        value_total = value_total + text_vpart

        def weight_block(running, section):
            block_grad, block_out = section
            term = jnp.dot(block_grad.T, block_out, preferred_element_type=jnp.float32)
            return running + lax.optimization_barrier(term.astype(jnp.bfloat16)).astype(jnp.float32), None

        weight_total, ignored = lax.scan(
            weight_block, jnp.zeros((upstream.shape[1], feature), jnp.float32),
            (upstream.reshape(N_SEQ, TOK_DEV, upstream.shape[1]), outputs.reshape(N_SEQ, TOK_DEV, feature)))
        return (query_blocks.reshape(length, feature).astype(jnp.bfloat16),
                key_total[:length].astype(jnp.bfloat16), value_total[:length].astype(jnp.bfloat16),
                text_qpart.astype(jnp.bfloat16), key_total[length:].astype(jnp.bfloat16),
                value_total[length:].astype(jnp.bfloat16), weight_total)

    results = lax.map(one_image, (image_query, image_key, image_value, image_output, output_grad, image_logsum,
                                  text_query, text_key, text_value, text_output, text_grad, text_logsum))
    return (results[0], results[1], results[2], results[3], results[4], results[5],
            jnp.sum(results[6], axis=0))
```

```python
import functools

import jax
import jax.numpy as jnp
from jax import lax
from jax.experimental import pallas as pl
from jax.experimental.pallas import tpu as pltpu
from jax.sharding import PartitionSpec as P

LANES = 128
SUB = 16
MESH = pl.DeviceIdType.MESH
NN = (((1,), (0,)), ((), ()))
NT = (((1,), (1,)), ((), ()))
TN = (((0,), (0,)), ((), ()))
BF = jnp.bfloat16
F32 = jnp.float32


def up(value, step):
    return -(-value // step) * step


class Plan:
    def __init__(self, peers, images, rows, text_rows, model, feature, heads):
        self.peers, self.images, self.rows = peers, images, rows
        self.text_rows, self.model, self.feature, self.heads = text_rows, model, feature, heads
        self.chips = peers // 2
        self.width = feature // heads
        self.depth = 2 * self.width
        self.most = -(-heads // peers)
        self.stat_rows = up(2 * self.most, 8)
        self.tokens = peers * rows
        self.total = self.tokens + up(text_rows, LANES)
        self.key_block = self.total // 8
        self.text_even = up(text_rows, SUB)
        self.text_half = up(self.text_even // 2, SUB)
        self.out_rows = rows + rows // 2
        self.out_text = self.text_even + self.text_half
        self.share = model // peers
        self.share_pad = up(self.share, SUB)
        self.part = up(-(-self.share_pad // images), SUB)

    def first(self, device):
        return device * self.heads // self.peers

    def part_start(self, image):
        if isinstance(image, int):
            return min(image * self.part, self.share_pad - self.part)
        return pl.multiple_of(jnp.minimum(image * self.part, self.share_pad - self.part), SUB)


def exchange_kernel(
    plan,
    q_ref, k_ref, v_ref, o_ref, og_ref, ls_ref,
    tq_ref, tk_ref, tv_ref, to_ref, tg_ref, tls_ref, w_ref,
    back_ref, tback_ref, parts_ref,
    w_s, txt_s, qk_out, gv_out, st_out, x_qk, x_gv, st_in, st_text, dots_s, tdots_s, stat_s,
    q_s, k_s, v_s, g_s, dk_s, dv_s, dq_s, result_s, ogt_s, og_in, io_in, sums_out, sums_in,
    local_sem, qk_send, qk_recv, gv_send, gv_recv, st_send, st_recv, back_send, back_recv,
    text_send, text_recv, io_send, io_recv, og_send, og_recv, sums_send, sums_recv,
    parts_send, parts_recv,
):
    p = plan
    peers, images, rows, width, depth, chips = p.peers, p.images, p.rows, p.width, p.depth, p.chips
    scaling = width ** (-0.5)
    me = lax.axis_index("seq")
    image = lax.axis_index("img")
    chip, core = me // 2, me % 2
    first = p.first(me)
    count = p.first(me + 1) - first
    slot = image * 2 + core
    my_rows = pl.ds(pl.multiple_of(me * rows, rows), rows)

    def remote(source, target, send, recv, device):
        return pltpu.make_async_remote_copy(
            src_ref=source, dst_ref=target, send_sem=send, recv_sem=recv,
            device_id=device, device_id_type=MESH,
        )

    loads = [
        pltpu.make_async_copy(ref, txt_s.at[number], local_sem.at[number])
        for number, ref in enumerate((tq_ref, tk_ref, tv_ref, tg_ref, to_ref))
    ]
    load_w = pltpu.make_async_copy(w_ref, w_s, local_sem.at[5])
    load_w.start()
    for load in loads:
        load.start()

    barrier = pltpu.get_barrier_semaphore()

    @pl.loop(1, peers)
    def _(step):
        pl.semaphore_signal(barrier, inc=1, device_id=(image, (me + step) % peers), device_id_type=MESH)

    @pl.loop(1, images)
    def _(step):
        for side in range(2):
            pl.semaphore_signal(
                barrier, inc=1, device_id=((image + step) % images, chip * 2 + side), device_id_type=MESH
            )

    for head in range(p.heads):
        cols = slice(head * width, (head + 1) * width)
        qk_out[head] = jnp.concatenate([q_ref[:, cols] * jnp.asarray(scaling, BF), k_ref[:, cols]], axis=1)

    pl.semaphore_wait(barrier, peers - 1 + 2 * (images - 1))

    def targets(j, action):
        @pl.loop(0, peers)
        def _(step):
            device = (me + peers // 2 + step) % peers
            head = p.first(device) + j

            @pl.when((device != me) & (head < p.first(device + 1)))
            def _():
                action(device, head)

    def copy_qk(j):
        return lambda device, head: remote(
            qk_out.at[head], x_qk.at[j, my_rows], qk_send.at[head], qk_recv.at[j], (image, device)
        )

    def copy_gv(j):
        return lambda device, head: remote(
            gv_out.at[head], x_gv.at[j, my_rows], gv_send.at[head], gv_recv.at[j], (image, device)
        )

    def copy_st(device):
        return remote(st_out.at[device], st_in.at[me], st_send.at[device], st_recv.at[me], (image, device))

    targets(0, lambda device, head: copy_qk(0)(device, head).start())

    def copy_io(step):
        return remote(
            o_ref, io_in.at[slot], io_send.at[step], io_recv.at[slot], ((image + step) % images, me)
        )

    def share_io(step):
        source = ((image + step) % images) * 2 + core
        return remote(
            io_in.at[source], io_in.at[source], io_send.at[images + step], io_recv.at[source],
            (image, chip * 2 + 1 - core),
        )

    copy_own = remote(
        o_ref, io_in.at[slot], io_send.at[0], io_recv.at[slot], (image, chip * 2 + 1 - core)
    )

    @pl.loop(1, images)
    def _(step):
        copy_io(step).start()

    copy_own.start()

    for number in range(-(-p.model // LANES)):
        lanes = slice(number * LANES, (number + 1) * LANES)
        dq_s[:, 0:rows] = jnp.zeros((LANES, rows), F32) + og_ref[:, lanes].astype(F32).T
        turned = dq_s[:, 0:rows]
        for device in range(peers):
            low = max(number * LANES, device * p.share)
            high = min((number + 1) * LANES, (device + 1) * p.share)
            if low < high:
                ogt_s[device % 2, device // 2, low - device * p.share : high - device * p.share, :] = turned[
                    low - number * LANES : high - number * LANES
                ].astype(BF)

    def copy_og(step, side):
        other = (image + step) % images
        return remote(
            ogt_s.at[side, :, pl.ds(p.part_start(other), p.part)],
            og_in.at[:, :, pl.ds(pl.multiple_of(slot * rows, rows), rows)],
            og_send.at[step, side],
            og_recv.at[slot],
            (other, chip * 2 + side),
        )

    @pl.loop(1, images)
    def _(step):
        for side in range(2):
            copy_og(step, side).start()

    for side in range(2):
        @pl.when(core != side)
        def _():
            copy_og(0, side).start()

    og_in[:, :, pl.ds(pl.multiple_of(slot * rows, rows), rows)] = ogt_s[
        core, :, pl.ds(p.part_start(image), p.part)
    ]
    io_in[slot] = o_ref[...]

    load_w.wait()

    @pl.loop(0, p.feature // 256)
    def _(step):
        lanes = pl.ds(pl.multiple_of(step * 256, 256), 256)
        g_cols = jnp.dot(og_ref[...], w_s[:, lanes], preferred_element_type=F32).astype(BF)
        per = 256 // width
        for number in range(per):
            head = step * per + number
            gv_out[head, :, 0:width] = g_cols[:, number * width : (number + 1) * width]

    pick_rows = up(p.heads, 8)
    tag = lax.broadcasted_iota(jnp.int32, (pick_rows, p.feature), 0)
    lane_at = lax.broadcasted_iota(jnp.int32, (pick_rows, p.feature), 1)
    picker = jnp.where((lane_at >= tag * width) & (lane_at < (tag + 1) * width), 1.0, 0.0).astype(F32)

    def row_dots(grads, outputs):
        product = grads.astype(F32) * outputs.astype(F32)
        return lax.dot_general(
            picker, product, NT, precision=lax.Precision.HIGHEST, preferred_element_type=F32
        )

    gathered = jnp.concatenate([gv_out[head, :, 0:width] for head in range(p.heads)], axis=1)
    dots_s[...] = row_dots(gathered, o_ref[...])
    for head in range(p.heads):
        gv_out[head, :, width:depth] = v_ref[:, head * width : (head + 1) * width]
    st_out[...] = jnp.zeros_like(st_out)
    for device in range(peers):
        for j in range(p.first(device + 1) - p.first(device)):
            head = p.first(device) + j
            st_out[device, 2 * j : 2 * j + 1, :] = -ls_ref[head : head + 1, :]
            st_out[device, 2 * j + 1 : 2 * j + 2, :] = -dots_s[head : head + 1, :]

    @pl.loop(0, peers)
    def _(step):
        device = (me + peers // 2 + step) % peers

        @pl.when(device != me)
        def _():
            copy_st(device).start()

    targets(0, lambda device, head: copy_gv(0)(device, head).start())
    for j in range(1, p.most):
        targets(j, lambda device, head: copy_qk(j)(device, head).start())
        targets(j, lambda device, head: copy_gv(j)(device, head).start())

    for load in loads:
        load.wait()
    tdots_s[...] = row_dots(txt_s[3], txt_s[4])
    st_text[...] = jnp.zeros_like(st_text)
    text_at = slice(p.tokens, p.tokens + p.text_rows)
    pad_at = slice(p.tokens + p.text_rows // SUB * SUB, p.total)

    @pl.loop(0, count)
    def _(j):
        head = first + j
        tile = pl.ds(pl.multiple_of(head // 2 * depth, depth), depth)
        odd = head % 2 == 1

        def text_cols(number):
            value = txt_s[number, :, tile]
            return jnp.where(odd, value[:, width:], value[:, :width])

        x_qk[j, my_rows] = qk_out[head]
        x_gv[j, my_rows] = gv_out[head]
        x_qk[j, pad_at] = jnp.zeros((p.total - pad_at.start, depth), BF)
        x_gv[j, pad_at] = jnp.zeros((p.total - pad_at.start, depth), BF)
        x_qk[j, text_at] = jnp.concatenate([text_cols(0) * jnp.asarray(scaling, BF), text_cols(1)], axis=1)
        x_gv[j, text_at] = jnp.concatenate([text_cols(3), text_cols(2)], axis=1)
        st_text[pl.ds(2 * j, 1), 0 : p.text_rows] = -tls_ref[pl.ds(head, 1), :]
        st_text[pl.ds(2 * j + 1, 1), 0 : p.text_rows] = -tdots_s[pl.ds(head, 1), :]

    def stats_tile(value):
        terms = []
        for _ in range(3):
            term = value.astype(BF).astype(F32)
            terms.append(term)
            value = value - term
        used = width + 3 * p.stat_rows
        return jnp.concatenate(
            [jnp.zeros((width, LANES), F32), *terms, jnp.zeros((depth - used, LANES), F32)], axis=0
        ).T.astype(BF)

    for number in range((p.total - p.tokens) // LANES):
        stat_s[p.tokens + number * LANES : p.tokens + (number + 1) * LANES, :] = stats_tile(
            st_text[:, number * LANES : (number + 1) * LANES]
        )

    st_in[me] = st_out[me]

    @pl.loop(1, peers)
    def _(step):
        source = (me + step) % peers
        remote(st_out.at[0], st_in.at[source], st_send.at[0], st_recv.at[source], (image, source)).wait_recv()

    @pl.loop(0, peers)
    def _(source):
        stat_s[pl.ds(pl.multiple_of(source * rows, rows), rows), :] = stats_tile(st_in[source])

    lane = lax.broadcasted_iota(jnp.int32, (p.total, depth), 1)

    def ones(start):
        inside = (lane == width + start)
        for number in range(1, 3):
            inside = inside | (lane == width + start + number * p.stat_rows)
        return jnp.where(inside, 1.0, 0.0).astype(BF)[:, width:]

    far = pl.ds(0, (peers - 1) * rows)

    def text_copy(head, way, device):
        return remote(
            tback_ref.at[head], tback_ref.at[head], text_send.at[head, way], text_recv.at[head], (image, device)
        )

    def send_text(head, upward, downward):
        @pl.when(upward & (chip + 1 < chips))
        def _():
            text_copy(head, 0, me + 2).start()

        @pl.when(downward & (chip > 0))
        def _():
            text_copy(head, 1, me - 2).start()

        text_copy(head, 2, chip * 2 + 1 - core).start()

    @pl.loop(0, count)
    def _(j):
        head = first + j
        pltpu.make_async_copy(x_qk.at[j, far], x_qk.at[j, far], qk_recv.at[j]).wait()
        pltpu.make_async_copy(x_gv.at[j, far], x_gv.at[j, far], gv_recv.at[j]).wait()
        both = x_qk[j]
        q_s[...] = jnp.where(lane < width, both, stat_s[...])
        k_s[...] = jnp.concatenate([both[:, width:], ones(2 * j)], axis=1)
        both = x_gv[j]
        g_s[...] = jnp.where(lane < width, both, stat_s[...])
        v_s[...] = jnp.concatenate([both[:, width:], ones(2 * j + 1)], axis=1)
        dq_s[...] = jnp.zeros_like(dq_s)

        @pl.loop(0, p.total // p.key_block)
        def _(step):
            at = pl.ds(pl.multiple_of(step * p.key_block, p.key_block), p.key_block)
            keys = k_s[at, :]
            scores = lax.dot_general(keys, q_s[...], NT, preferred_element_type=F32)
            weights = jnp.exp(scores)
            grads = lax.dot_general(v_s[at, :], g_s[...], NT, preferred_element_type=F32)
            low = (weights * grads).astype(BF)
            dv_s[at, :] = jnp.dot(weights.astype(BF), g_s[...], preferred_element_type=F32).astype(BF)
            dk_s[at, :] = jnp.dot(low, q_s[...], preferred_element_type=F32).astype(BF)
            dq_s[...] += lax.dot_general(keys, low, TN, preferred_element_type=F32)

        @pl.loop(0, peers)
        def _(block):
            base = pl.multiple_of(block * rows, rows)
            dq = (dq_s[:, pl.ds(base, rows)].T * scaling).astype(BF)
            top = jnp.concatenate([dq[:, :width], dk_s[pl.ds(base, rows), :width]], axis=1)
            dv = dv_s[pl.ds(base, rows), :width]
            bottom = jnp.concatenate([dv[: rows // 2], dv[rows // 2 :]], axis=1)
            result_s[j, block, 0:rows] = top
            result_s[j, block, rows : p.out_rows] = bottom

            @pl.when(block == me)
            def _():
                back_ref[head, 0:rows] = top
                back_ref[head, rows : p.out_rows] = bottom

            @pl.when(block != me)
            def _():
                remote(
                    result_s.at[j, block], back_ref.at[head], back_send.at[j, block], back_recv.at[head],
                    (image, block),
                ).start()

        dq = (dq_s[:, p.tokens : p.total].T * scaling).astype(BF)
        even, half = p.text_even, p.text_half
        tback_ref[head, 0:even] = jnp.concatenate(
            [dq[:even, :width], dk_s[p.tokens : p.tokens + even, :width]], axis=1
        )
        tback_ref[head, even : even + half] = jnp.concatenate(
            [dv_s[p.tokens : p.tokens + half, :width], dv_s[p.tokens + half : p.tokens + 2 * half, :width]],
            axis=1,
        )
        send_text(head, True, True)

        @pl.when(j == 0)
        def _():
            @pl.loop(1, images)
            def _(step):
                source = ((image + step) % images) * 2 + core
                pltpu.make_async_copy(io_in.at[source], io_in.at[source], io_recv.at[source]).wait()
                share_io(step).start()

        @pl.when(j == jnp.minimum(1, count - 1))
        def _():
            @pl.loop(0, images)
            def _(index):
                source = index * 2 + 1 - core
                pltpu.make_async_copy(io_in.at[source], io_in.at[source], io_recv.at[source]).wait()

            @pl.loop(1, 2 * images)
            def _(step):
                source = (slot + step) % (2 * images)
                piece = og_in.at[:, :, pl.ds(pl.multiple_of(source * rows, rows), rows)]
                pltpu.make_async_copy(piece, piece, og_recv.at[source]).wait()

            @pl.loop(0, p.feature // 256)
            def _(step):
                lanes = pl.ds(pl.multiple_of(step * 256, 256), 256)
                for number in range(chips):
                    total = jnp.zeros((p.part, 256), F32)
                    for source in range(2 * images):
                        total += jnp.dot(
                            og_in[number, :, source * rows : (source + 1) * rows],
                            io_in[source, :, lanes],
                            preferred_element_type=F32,
                        )
                    sums_out[number, :, lanes] = total.astype(BF)

            @pl.loop(0, chips)
            def _(number):
                @pl.when(number != chip)
                def _():
                    remote(
                        sums_out.at[number], sums_in.at[chip], sums_send.at[number], sums_recv.at[chip],
                        (image, number * 2 + core),
                    ).start()

            sums_in[chip] = sums_out[chip]

    @pl.loop(1, chips)
    def _(hop):
        for upward in (True, False):
            source = chip - hop if upward else chip + hop

            @pl.when((source >= 0) & (source < chips))
            def _():
                owner = source * 2 + core
                start = p.first(owner)

                @pl.loop(start, p.first(owner + 1))
                def _(head):
                    pltpu.make_async_copy(tback_ref.at[head], tback_ref.at[head], text_recv.at[head]).wait()
                    send_text(head, upward, not upward)

    @pl.loop(1, chips)
    def _(step):
        source = (chip + step) % chips
        pltpu.make_async_copy(sums_in.at[source], sums_in.at[source], sums_recv.at[source]).wait()

    @pl.loop(0, p.feature // 256)
    def _(step):
        lanes = pl.ds(pl.multiple_of(step * 256, 256), 256)
        total = sums_in[0, :, lanes].astype(F32)
        for source in range(1, chips):
            total += sums_in[source, :, lanes].astype(F32)
        parts_ref[image, :, lanes] = total.astype(BF)

    def copy_parts(step):
        return remote(
            parts_ref.at[image], parts_ref.at[image], parts_send.at[step], parts_recv.at[image],
            ((image + step) % images, me),
        )

    @pl.loop(1, images)
    def _(step):
        copy_parts(step).start()

    @pl.loop(0, p.heads)
    def _(head):
        @pl.when((head < first) | (head >= first + count))
        def _():
            pltpu.make_async_copy(back_ref.at[head], back_ref.at[head], back_recv.at[head]).wait()
            pltpu.make_async_copy(qk_out.at[head], qk_out.at[head], qk_send.at[head]).wait()
            pltpu.make_async_copy(gv_out.at[head], gv_out.at[head], gv_send.at[head]).wait()

    @pl.loop(0, chips)
    def _(number):
        owner = number * 2 + 1 - core

        @pl.loop(p.first(owner), p.first(owner + 1))
        def _(head):
            pltpu.make_async_copy(tback_ref.at[head], tback_ref.at[head], text_recv.at[head]).wait()

        owner = number * 2 + core

        @pl.loop(p.first(owner), p.first(owner + 1))
        def _(head):
            @pl.when((number <= chip) & (chip + 1 < chips))
            def _():
                text_copy(head, 0, me).wait_send()

            @pl.when((number >= chip) & (chip > 0))
            def _():
                text_copy(head, 1, me).wait_send()

            text_copy(head, 2, me).wait_send()

        @pl.when(number != chip)
        def _():
            pltpu.make_async_copy(sums_out.at[number], sums_out.at[number], sums_send.at[number]).wait()

    @pl.loop(0, peers)
    def _(device):
        @pl.when(device != me)
        def _():
            pltpu.make_async_copy(st_out.at[device], st_out.at[device], st_send.at[device]).wait()

            @pl.loop(0, count)
            def _(j):
                piece = result_s.at[j, device]
                pltpu.make_async_copy(piece, piece, back_send.at[j, device]).wait()

    copy_own.wait_send()
    for side in range(2):
        @pl.when(core != side)
        def _():
            copy_og(0, side).wait_send()

    @pl.loop(1, images)
    def _(step):
        copy_io(step).wait_send()
        share_io(step).wait_send()
        copy_parts(step).wait_send()
        for side in range(2):
            copy_og(step, side).wait_send()
        source = (image + step) % images
        pltpu.make_async_copy(parts_ref.at[source], parts_ref.at[source], parts_recv.at[source]).wait()


def exchange(plan, *arrays):
    p = plan
    dma = pltpu.SemaphoreType.DMA
    vmem = pl.BlockSpec(memory_space=pltpu.VMEM)
    anywhere = pl.BlockSpec(memory_space=pl.ANY)
    pick = up(p.heads, 8)
    wide = (p.total, p.depth)
    return pl.pallas_call(
        functools.partial(exchange_kernel, p),
        out_shape=(
            jax.ShapeDtypeStruct((p.heads, p.out_rows, p.depth), BF),
            jax.ShapeDtypeStruct((p.heads, p.out_text, p.depth), BF),
            jax.ShapeDtypeStruct((p.images, p.part, p.feature), BF),
        ),
        in_specs=[vmem] * 6 + [anywhere] * 5 + [vmem, anywhere],
        out_specs=(vmem,) * 3,
        scratch_shapes=[
            pltpu.VMEM((p.model, p.feature), BF),
            pltpu.VMEM((5, p.text_rows, p.feature), BF),
            pltpu.VMEM((p.heads, p.rows, p.depth), BF),
            pltpu.VMEM((p.heads, p.rows, p.depth), BF),
            pltpu.VMEM((p.peers, p.stat_rows, p.rows), F32),
            pltpu.VMEM((p.most, *wide), BF),
            pltpu.VMEM((p.most, *wide), BF),
            pltpu.VMEM((p.peers, p.stat_rows, p.rows), F32),
            pltpu.VMEM((p.stat_rows, p.total - p.tokens), F32),
            pltpu.VMEM((pick, p.rows), F32),
            pltpu.VMEM((pick, p.text_rows), F32),
            pltpu.VMEM(wide, BF),
        ]
        + [pltpu.VMEM(wide, BF)] * 6
        + [
            pltpu.VMEM((p.depth, p.total), F32),
            pltpu.VMEM((p.most, p.peers, p.out_rows, p.depth), BF),
            pltpu.VMEM((2, p.chips, p.share_pad, p.rows), BF),
            pltpu.VMEM((p.chips, p.part, 2 * p.images * p.rows), BF),
            pltpu.VMEM((2 * p.images, p.rows, p.feature), BF),
            pltpu.VMEM((p.chips, p.part, p.feature), BF),
            pltpu.VMEM((p.chips, p.part, p.feature), BF),
            dma((6,)),
            dma((p.heads,)), dma((p.most,)),
            dma((p.heads,)), dma((p.most,)),
            dma((p.peers,)), dma((p.peers,)),
            dma((p.most, p.peers)), dma((p.heads,)),
            dma((p.heads, 3)), dma((p.heads,)),
            dma((2 * p.images,)), dma((2 * p.images,)),
            dma((p.images, 2)), dma((2 * p.images,)),
            dma((p.chips,)), dma((p.chips,)),
            dma((p.images,)), dma((p.images,)),
        ],
        compiler_params=pltpu.CompilerParams(
            collective_id=0, has_side_effects=True, vmem_limit_bytes=60 << 20
        ),
    )(*arrays)


def finish_kernel(plan, back_ref, tback_ref, parts_ref, dq_ref, dk_ref, dv_ref, tdq_ref, tdk_ref, tdv_ref, wg_ref):
    p = plan
    width, rows, half, even = p.width, p.rows, p.text_half, p.text_even
    for pair in range(p.heads // 2):
        lanes = slice(pair * p.depth, (pair + 1) * p.depth)

        def join(ref, at, cols):
            return jnp.concatenate([ref[2 * pair, at, cols], ref[2 * pair + 1, at, cols]], axis=1)

        left, right = slice(0, width), slice(width, p.depth)
        dq_ref[:, lanes] = join(back_ref, slice(0, rows), left)
        dk_ref[:, lanes] = join(back_ref, slice(0, rows), right)
        dv_ref[0 : rows // 2, lanes] = join(back_ref, slice(rows, p.out_rows), left)
        dv_ref[rows // 2 : rows, lanes] = join(back_ref, slice(rows, p.out_rows), right)
        tdq_ref[:, lanes] = join(tback_ref, slice(0, p.text_rows), left)
        tdk_ref[:, lanes] = join(tback_ref, slice(0, p.text_rows), right)
        tdv_ref[0:half, lanes] = join(tback_ref, slice(even, even + half), left)
        tdv_ref[half : p.text_rows, lanes] = join(tback_ref, slice(even, even + p.text_rows - half), right)
    for number in range(p.images):
        start = p.part_start(number)
        stop = min(start + p.part, p.share)
        wg_ref[start:stop, :] = parts_ref[number, 0 : stop - start, :].astype(F32)


def finish(plan, back, tback, parts):
    p = plan
    vmem = pl.BlockSpec(memory_space=pltpu.VMEM)
    token = jax.ShapeDtypeStruct((p.rows, p.feature), BF)
    text = jax.ShapeDtypeStruct((p.text_rows, p.feature), BF)
    return pl.pallas_call(
        functools.partial(finish_kernel, p),
        out_shape=(token,) * 3 + (text,) * 3 + (jax.ShapeDtypeStruct((p.share, p.feature), F32),),
        in_specs=[vmem] * 3,
        out_specs=(vmem,) * 7,
        compiler_params=pltpu.CompilerParams(vmem_limit_bytes=40 << 20),
    )(back, tback, parts)


def shards(
    image_query,
    image_key,
    image_value,
    image_output,
    output_grad,
    image_logsum,
    text_query,
    text_key,
    text_value,
    text_output,
    text_grad,
    text_logsum,
    out_weight,
):
    plan = Plan(
        lax.axis_size("seq"),
        lax.axis_size("img"),
        image_query.shape[1],
        text_query.shape[1],
        output_grad.shape[2],
        image_query.shape[2],
        image_logsum.shape[2],
    )
    results = exchange(
        plan,
        image_query[0], image_key[0], image_value[0], image_output[0], output_grad[0], image_logsum[0].T,
        text_query[0], text_key[0], text_value[0], text_output[0], text_grad[0], text_logsum[0].T,
        out_weight,
    )
    *grads, weight_grad = finish(plan, *results)
    return (*(grad[None] for grad in grads), weight_grad)


def solution(mesh):
    token = P("img", "seq", None)
    text = P("img", None, None)
    return jax.shard_map(
        shards,
        mesh=mesh,
        in_specs=(token,) * 6 + (text,) * 6 + (P(),),
        out_specs=(token,) * 3 + (text,) * 3 + (P("seq", None),),
        check_vma=False,
    )
```

```python
import functools

import jax
import jax.numpy as jnp
from jax import lax
from jax.experimental import pallas as pl
from jax.experimental.pallas import tpu as pltpu
from jax.sharding import PartitionSpec as P

LANES = 128
SUB = 16
MESH = pl.DeviceIdType.MESH
NN = (((1,), (0,)), ((), ()))
NT = (((1,), (1,)), ((), ()))
TN = (((0,), (0,)), ((), ()))
BF = jnp.bfloat16
F32 = jnp.float32


def up(value, step):
    return -(-value // step) * step


class Plan:
    def __init__(self, peers, images, rows, text_rows, model, feature, heads):
        self.peers, self.images, self.rows = peers, images, rows
        self.text_rows, self.model, self.feature, self.heads = text_rows, model, feature, heads
        self.chips = peers // 2
        self.width = feature // heads
        self.depth = 2 * self.width
        self.most = -(-heads // peers)
        self.stat_rows = up(2 * self.most, 8)
        self.tokens = peers * rows
        self.total = self.tokens + up(text_rows, LANES)
        self.key_block = self.total // 8
        self.text_even = up(text_rows, SUB)
        self.text_half = up(self.text_even // 2, SUB)
        self.out_rows = rows + rows // 2
        self.out_text = self.text_even + self.text_half
        self.share = model // peers
        self.finish_steps = next(n for n in (5, 4, 3, 2, 1) if heads % (2 * n) == 0)
        self.share_pad = up(self.share, SUB)
        self.part = up(-(-self.share_pad // images), SUB)

    def first(self, device):
        return device * self.heads // self.peers

    def part_start(self, image):
        if isinstance(image, int):
            return min(image * self.part, self.share_pad - self.part)
        return pl.multiple_of(jnp.minimum(image * self.part, self.share_pad - self.part), SUB)


def exchange_kernel(
    plan,
    q_in, k_in, v_in, o_in, og_in_ref, ls_in,
    tq_ref, tk_ref, tv_ref, to_ref, tg_ref, tls_in, w_ref,
    back_ref, tback_ref, parts_ref,
    q_ref, k_ref, v_ref, o_ref, og_ref, ls_ref, tls_ref, text_s, w_s, txt_s, qk_out, gv_out, st_out, x_qk, x_gv, st_in, st_text, dots_s, tdots_s, stat_s,
    q_s, k_s, v_s, g_s, dk_s, dv_s, dq_s, result_s, ogt_s, og_in, io_in, sums_out, sums_in, gate_in,
    local_sem, own_sem, qk_send, qk_recv, gv_send, gv_recv, st_send, st_recv, back_send, back_recv,
    text_send, text_recv, io_send, io_recv, og_send, og_recv, sums_send, sums_recv, gate_recv,
    parts_send, parts_recv,
):
    p = plan
    peers, images, rows, width, depth, chips = p.peers, p.images, p.rows, p.width, p.depth, p.chips
    scaling = width ** (-0.5)
    me = lax.axis_index("seq")
    image = lax.axis_index("img")
    chip, core = me // 2, me % 2
    first = p.first(me)
    count = p.first(me + 1) - first
    slot = image * 2 + core
    my_rows = pl.ds(pl.multiple_of(me * rows, rows), rows)

    def remote(source, target, send, recv, device):
        return pltpu.make_async_remote_copy(
            src_ref=source, dst_ref=target, send_sem=send, recv_sem=recv,
            device_id=device, device_id_type=MESH,
        )

    barrier = pltpu.get_barrier_semaphore()

    @pl.loop(1, peers)
    def _(step):
        pl.semaphore_signal(barrier, inc=1, device_id=(image, (me + step) % peers), device_id_type=MESH)

    @pl.loop(1, images)
    def _(step):
        for side in range(2):
            pl.semaphore_signal(
                barrier, inc=1, device_id=((image + step) % images, chip * 2 + side), device_id_type=MESH
            )

    names = ("q", "k", "o", "og", "w", "v", "ls", "tq", "tk", "tv", "tg", "to", "tls")
    pairs = (
        (q_in, q_ref), (k_in, k_ref), (o_in, o_ref), (og_in_ref, og_ref), (w_ref, w_s), (v_in, v_ref), (ls_in, ls_ref),
        (tq_ref, txt_s.at[0]), (tk_ref, txt_s.at[1]), (tv_ref, txt_s.at[2]), (tg_ref, txt_s.at[3]),
        (to_ref, txt_s.at[4]), (tls_in, tls_ref),
    )
    loads = {}
    for number, (name, (source, target)) in enumerate(zip(names, pairs)):
        loads[name] = pltpu.make_async_copy(source, target, local_sem.at[number])
        loads[name].start()

    loads["q"].wait()
    loads["k"].wait()

    for head in range(p.heads):
        cols = slice(head * width, (head + 1) * width)
        qk_out[head] = jnp.concatenate([q_ref[:, cols] * jnp.asarray(scaling, BF), k_ref[:, cols]], axis=1)

    pl.semaphore_wait(barrier, peers - 1 + 2 * (images - 1))

    def targets(j, action):
        @pl.loop(0, peers)
        def _(step):
            device = (me + peers // 2 + step) % peers
            head = p.first(device) + j

            @pl.when((device != me) & (head < p.first(device + 1)))
            def _():
                action(device, head)

    def copy_qk(j):
        return lambda device, head: remote(
            qk_out.at[head], x_qk.at[j, my_rows], qk_send.at[head], qk_recv.at[j], (image, device)
        )

    def copy_gv(j):
        return lambda device, head: remote(
            gv_out.at[head], x_gv.at[j, my_rows], gv_send.at[head], gv_recv.at[j], (image, device)
        )

    def copy_st(device):
        return remote(st_out.at[device], st_in.at[me], st_send.at[device], st_recv.at[me], (image, device))

    targets(0, lambda device, head: copy_qk(0)(device, head).start())

    loads["o"].wait()
    loads["og"].wait()

    def copy_io(step):
        return remote(
            o_ref, io_in.at[slot], io_send.at[step], io_recv.at[slot], ((image + step) % images, me)
        )

    def share_io(step):
        source = ((image + step) % images) * 2 + core
        return remote(
            io_in.at[source], io_in.at[source], io_send.at[images + step], io_recv.at[source],
            (image, chip * 2 + 1 - core),
        )

    copy_own = remote(
        o_ref, io_in.at[slot], io_send.at[0], io_recv.at[slot], (image, chip * 2 + 1 - core)
    )

    @pl.loop(1, images)
    def _(step):
        copy_io(step).start()

    copy_own.start()

    for number in range(-(-p.model // LANES)):
        lanes = slice(number * LANES, (number + 1) * LANES)
        dq_s[:, 0:rows] = jnp.zeros((LANES, rows), F32) + og_ref[:, lanes].astype(F32).T
        turned = dq_s[:, 0:rows]
        for device in range(peers):
            low = max(number * LANES, device * p.share)
            high = min((number + 1) * LANES, (device + 1) * p.share)
            if low < high:
                ogt_s[device % 2, device // 2, low - device * p.share : high - device * p.share, :] = turned[
                    low - number * LANES : high - number * LANES
                ].astype(BF)

    def copy_og(step, side):
        other = (image + step) % images
        return remote(
            ogt_s.at[side, :, pl.ds(p.part_start(other), p.part)],
            og_in.at[:, :, pl.ds(pl.multiple_of(slot * rows, rows), rows)],
            og_send.at[step, side],
            og_recv.at[slot],
            (other, chip * 2 + side),
        )

    @pl.loop(1, images)
    def _(step):
        for side in range(2):
            copy_og(step, side).start()

    for side in range(2):
        @pl.when(core != side)
        def _():
            copy_og(0, side).start()

    og_in[:, :, pl.ds(pl.multiple_of(slot * rows, rows), rows)] = ogt_s[
        core, :, pl.ds(p.part_start(image), p.part)
    ]
    io_in[slot] = o_ref[...]

    loads["w"].wait()

    @pl.loop(0, p.feature // 256)
    def _(step):
        lanes = pl.ds(pl.multiple_of(step * 256, 256), 256)
        g_cols = jnp.dot(og_ref[...], w_s[:, lanes], preferred_element_type=F32).astype(BF)
        per = 256 // width
        for number in range(per):
            head = step * per + number
            gv_out[head, :, 0:width] = g_cols[:, number * width : (number + 1) * width]

    pick_rows = up(p.heads, 8)
    tag = lax.broadcasted_iota(jnp.int32, (pick_rows, p.feature), 0)
    lane_at = lax.broadcasted_iota(jnp.int32, (pick_rows, p.feature), 1)
    picker = jnp.where((lane_at >= tag * width) & (lane_at < (tag + 1) * width), 1.0, 0.0).astype(F32)

    def row_dots(grads, outputs):
        product = grads.astype(F32) * outputs.astype(F32)
        return lax.dot_general(
            picker, product, NT, precision=lax.Precision.HIGHEST, preferred_element_type=F32
        )

    gathered = jnp.concatenate([gv_out[head, :, 0:width] for head in range(p.heads)], axis=1)
    dots_s[...] = row_dots(gathered, o_ref[...])
    loads["v"].wait()
    loads["ls"].wait()
    for head in range(p.heads):
        gv_out[head, :, width:depth] = v_ref[:, head * width : (head + 1) * width]
    st_out[...] = jnp.zeros_like(st_out)
    for device in range(peers):
        for j in range(p.first(device + 1) - p.first(device)):
            head = p.first(device) + j
            st_out[device, 2 * j : 2 * j + 1, :] = -ls_ref[head]
            st_out[device, 2 * j + 1 : 2 * j + 2, :] = -dots_s[head : head + 1, :]

    @pl.loop(0, peers)
    def _(step):
        device = (me + peers // 2 + step) % peers

        @pl.when(device != me)
        def _():
            copy_st(device).start()

    targets(0, lambda device, head: copy_gv(0)(device, head).start())
    for j in range(1, p.most):
        targets(j, lambda device, head: copy_qk(j)(device, head).start())
        targets(j, lambda device, head: copy_gv(j)(device, head).start())

    for name in names[7:]:
        loads[name].wait()
    tdots_s[...] = row_dots(txt_s[3], txt_s[4])
    st_text[...] = jnp.zeros_like(st_text)
    text_at = slice(p.tokens, p.tokens + p.text_rows)
    pad_at = slice(p.tokens + p.text_rows // SUB * SUB, p.total)

    @pl.loop(0, count)
    def _(j):
        head = first + j
        tile = pl.ds(pl.multiple_of(head // 2 * depth, depth), depth)
        odd = head % 2 == 1

        def text_cols(number):
            value = txt_s[number, :, tile]
            return jnp.where(odd, value[:, width:], value[:, :width])

        x_qk[j, my_rows] = qk_out[head]
        x_gv[j, my_rows] = gv_out[head]
        x_qk[j, pad_at] = jnp.zeros((p.total - pad_at.start, depth), BF)
        x_gv[j, pad_at] = jnp.zeros((p.total - pad_at.start, depth), BF)
        x_qk[j, text_at] = jnp.concatenate([text_cols(0) * jnp.asarray(scaling, BF), text_cols(1)], axis=1)
        x_gv[j, text_at] = jnp.concatenate([text_cols(3), text_cols(2)], axis=1)
        st_text[pl.ds(2 * j, 1), 0 : p.text_rows] = -tls_ref[head]
        st_text[pl.ds(2 * j + 1, 1), 0 : p.text_rows] = -tdots_s[pl.ds(head, 1), :]

    def stats_tile(value):
        terms = []
        for _ in range(3):
            term = value.astype(BF).astype(F32)
            terms.append(term)
            value = value - term
        used = width + 3 * p.stat_rows
        return jnp.concatenate(
            [jnp.zeros((width, LANES), F32), *terms, jnp.zeros((depth - used, LANES), F32)], axis=0
        ).T.astype(BF)

    for number in range((p.total - p.tokens) // LANES):
        stat_s[p.tokens + number * LANES : p.tokens + (number + 1) * LANES, :] = stats_tile(
            st_text[:, number * LANES : (number + 1) * LANES]
        )

    st_in[me] = st_out[me]

    @pl.loop(1, peers)
    def _(step):
        source = (me + step) % peers
        remote(st_out.at[0], st_in.at[source], st_send.at[0], st_recv.at[source], (image, source)).wait_recv()

    @pl.loop(0, peers)
    def _(source):
        stat_s[pl.ds(pl.multiple_of(source * rows, rows), rows), :] = stats_tile(st_in[source])

    lane = lax.broadcasted_iota(jnp.int32, (p.total, depth), 1)

    def ones(start):
        inside = (lane == width + start)
        for number in range(1, 3):
            inside = inside | (lane == width + start + number * p.stat_rows)
        return jnp.where(inside, 1.0, 0.0).astype(BF)[:, width:]

    far = pl.ds(0, (peers - 1) * rows)

    def text_copy(source, head, way, device):
        return remote(source, tback_ref.at[head], text_send.at[head, way], text_recv.at[head], (image, device))

    def send_text(source, head, upward, downward):
        @pl.when(upward & (chip + 1 < chips))
        def _():
            text_copy(source, head, 0, me + 2).start()

        @pl.when(downward & (chip > 0))
        def _():
            text_copy(source, head, 1, me - 2).start()

        text_copy(source, head, 2, chip * 2 + 1 - core).start()

    def own_back(j):
        return pltpu.make_async_copy(result_s.at[j, me], back_ref.at[first + j], own_sem.at[0, j])

    def send_back(j):
        own_back(j).start()

        @pl.loop(0, peers)
        def _(step):
            block = (me + peers // 2 + step) % peers

            @pl.when(block != me)
            def _():
                remote(
                    result_s.at[j, block], back_ref.at[first + j], back_send.at[j, block],
                    back_recv.at[first + j], (image, block),
                ).start()

    def own_text(j):
        return pltpu.make_async_copy(text_s.at[j], tback_ref.at[first + j], own_sem.at[1, j])

    half_chips = chips // 2
    side, seat = chip // half_chips, chip % half_chips
    gate = half_chips - 1 + side
    near, beyond = side * half_chips, (1 - side) * half_chips
    edge = chip != gate

    def send_sum(number, target, recv, device):
        remote(
            sums_out.at[number], target, sums_send.at[number], recv, (image, device * 2 + core)
        ).start()

    def send_terms():
        for number in range(half_chips):
            @pl.when(edge)
            def _():
                send_sum(beyond + number, gate_in.at[seat, number], gate_recv.at[seat, number], gate)

        for number in range(half_chips):
            @pl.when(number != seat)
            def _():
                send_sum(near + number, sums_in.at[seat], sums_recv.at[seat], near + number)

    def pass_sums():
        @pl.when(chip == gate)
        def _():
            for number in range(half_chips):
                @pl.loop(1, half_chips)
                def _(step):
                    source = (seat + step) % half_chips
                    piece = gate_in.at[source, number]
                    pltpu.make_async_copy(piece, piece, gate_recv.at[source, number]).wait()

                    @pl.loop(0, p.feature // 256)
                    def _(step):
                        lanes = pl.ds(pl.multiple_of(step * 256, 256), 256)
                        total = sums_out[beyond + number, :, lanes].astype(F32)
                        total += gate_in[source, number, :, lanes].astype(F32)
                        sums_out[beyond + number, :, lanes] = total.astype(BF)

                send_sum(beyond + number, sums_in.at[half_chips], sums_recv.at[half_chips], beyond + number)

    def pass_text(hop, low, high):
        for upward in (True, False):
            source = chip - hop if upward else chip + hop

            @pl.when((source >= 0) & (source < chips))
            def _():
                owner = source * 2 + core
                start, stop = p.first(owner), p.first(owner + 1)

                @pl.loop(start + low, jnp.minimum(stop, start + high))
                def _(head):
                    pltpu.make_async_copy(tback_ref.at[head], tback_ref.at[head], text_recv.at[head]).wait()
                    send_text(tback_ref.at[head], head, upward, not upward)

    @pl.loop(0, count)
    def _(j):
        head = first + j
        pltpu.make_async_copy(x_qk.at[j, far], x_qk.at[j, far], qk_recv.at[j]).wait()
        pltpu.make_async_copy(x_gv.at[j, far], x_gv.at[j, far], gv_recv.at[j]).wait()
        both = x_qk[j]
        q_s[...] = jnp.where(lane < width, both, stat_s[...])
        k_s[...] = jnp.concatenate([both[:, width:], ones(2 * j)], axis=1)
        both = x_gv[j]
        g_s[...] = jnp.where(lane < width, both, stat_s[...])
        v_s[...] = jnp.concatenate([both[:, width:], ones(2 * j + 1)], axis=1)
        dq_s[...] = jnp.zeros_like(dq_s)

        @pl.loop(0, p.total // p.key_block)
        def _(step):
            at = pl.ds(pl.multiple_of(step * p.key_block, p.key_block), p.key_block)
            keys = k_s[at, :]
            scores = lax.dot_general(keys, q_s[...], NT, preferred_element_type=F32)
            weights = jnp.exp(scores)
            grads = lax.dot_general(v_s[at, :], g_s[...], NT, preferred_element_type=F32)
            low = (weights * grads).astype(BF)
            dv_s[at, :] = jnp.dot(weights.astype(BF), g_s[...], preferred_element_type=F32).astype(BF)
            dk_s[at, :] = jnp.dot(low, q_s[...], preferred_element_type=F32).astype(BF)
            dq_s[...] += lax.dot_general(keys, low, TN, preferred_element_type=F32)

        dq = (dq_s[:, p.tokens : p.total].T * scaling).astype(BF)
        even, half = p.text_even, p.text_half
        text_s[j, 0:even] = jnp.concatenate(
            [dq[:even, :width], dk_s[p.tokens : p.tokens + even, :width]], axis=1
        )
        text_s[j, even : even + half] = jnp.concatenate(
            [dv_s[p.tokens : p.tokens + half, :width], dv_s[p.tokens + half : p.tokens + 2 * half, :width]],
            axis=1,
        )
        own_text(j).start()
        send_text(text_s.at[j], head, True, True)

        @pl.when(j == 0)
        def _():
            @pl.loop(1, images)
            def _(step):
                source = ((image + step) % images) * 2 + core
                pltpu.make_async_copy(io_in.at[source], io_in.at[source], io_recv.at[source]).wait()
                share_io(step).start()

        @pl.when(j == 0)
        def _():
            @pl.loop(0, images)
            def _(index):
                source = index * 2 + 1 - core
                pltpu.make_async_copy(io_in.at[source], io_in.at[source], io_recv.at[source]).wait()

            @pl.loop(1, 2 * images)
            def _(step):
                source = (slot + step) % (2 * images)
                piece = og_in.at[:, :, pl.ds(pl.multiple_of(source * rows, rows), rows)]
                pltpu.make_async_copy(piece, piece, og_recv.at[source]).wait()

            @pl.loop(0, p.feature // 256)
            def _(step):
                lanes = pl.ds(pl.multiple_of(step * 256, 256), 256)
                for number in range(chips):
                    total = jnp.zeros((p.part, 256), F32)
                    for source in range(2 * images):
                        total += jnp.dot(
                            og_in[number, :, source * rows : (source + 1) * rows],
                            io_in[source, :, lanes],
                            preferred_element_type=F32,
                        )
                    sums_out[number, :, lanes] = total.astype(BF)

            send_terms()

        @pl.loop(0, peers)
        def _(block):
            base = pl.multiple_of(block * rows, rows)
            dq = (dq_s[:, pl.ds(base, rows)].T * scaling).astype(BF)
            top = jnp.concatenate([dq[:, :width], dk_s[pl.ds(base, rows), :width]], axis=1)
            dv = dv_s[pl.ds(base, rows), :width]
            bottom = jnp.concatenate([dv[: rows // 2], dv[rows // 2 :]], axis=1)
            result_s[j, block, 0:rows] = top
            result_s[j, block, rows : p.out_rows] = bottom

        @pl.when(j == 0)
        def _():
            pass_text(1, 0, 1)

        @pl.when(j == jnp.minimum(1, count - 1))
        def _():
            pass_sums()

        late = jnp.where(edge, 1, 0)

        @pl.when(j >= late)
        def _():
            send_back(j - late)


    pass_text(1, 1, p.most)

    @pl.when(edge)
    def _():
        send_back(count - 1)

    @pl.loop(0, half_chips + 1)
    def _(source):
        @pl.when(source != seat)
        def _():
            pltpu.make_async_copy(sums_in.at[source], sums_in.at[source], sums_recv.at[source]).wait()

    @pl.loop(0, half_chips + 1)
    def _(source):
        @pl.when(source != seat)
        def _():
            @pl.loop(0, p.feature // 256)
            def _(step):
                lanes = pl.ds(pl.multiple_of(step * 256, 256), 256)
                total = sums_out[chip, :, lanes].astype(F32) + sums_in[source, :, lanes].astype(F32)
                sums_out[chip, :, lanes] = total.astype(BF)

    own_parts = pltpu.make_async_copy(sums_out.at[chip], parts_ref.at[image], own_sem.at[0, p.most])
    own_parts.start()

    def copy_parts(step):
        return remote(
            sums_out.at[chip], parts_ref.at[image], parts_send.at[step], parts_recv.at[image],
            ((image + step) % images, me),
        )

    @pl.loop(1, images)
    def _(step):
        copy_parts(step).start()

    for hop in range(2, chips):
        pass_text(hop, 0, p.most)

    @pl.loop(0, p.heads)
    def _(head):
        @pl.when((head < first) | (head >= first + count))
        def _():
            pltpu.make_async_copy(back_ref.at[head], back_ref.at[head], back_recv.at[head]).wait()
            pltpu.make_async_copy(qk_out.at[head], qk_out.at[head], qk_send.at[head]).wait()
            pltpu.make_async_copy(gv_out.at[head], gv_out.at[head], gv_send.at[head]).wait()

    @pl.loop(0, chips)
    def _(number):
        owner = number * 2 + 1 - core

        @pl.loop(p.first(owner), p.first(owner + 1))
        def _(head):
            pltpu.make_async_copy(tback_ref.at[head], tback_ref.at[head], text_recv.at[head]).wait()

        owner = number * 2 + core

        @pl.loop(p.first(owner), p.first(owner + 1))
        def _(head):
            @pl.when((number <= chip) & (chip + 1 < chips))
            def _():
                text_copy(tback_ref.at[head], head, 0, me).wait_send()

            @pl.when((number >= chip) & (chip > 0))
            def _():
                text_copy(tback_ref.at[head], head, 1, me).wait_send()

            text_copy(tback_ref.at[head], head, 2, me).wait_send()

        @pl.when(number != chip)
        def _():
            pltpu.make_async_copy(sums_out.at[number], sums_out.at[number], sums_send.at[number]).wait()

    @pl.loop(0, peers)
    def _(device):
        @pl.when(device != me)
        def _():
            pltpu.make_async_copy(st_out.at[device], st_out.at[device], st_send.at[device]).wait()

            @pl.loop(0, count)
            def _(j):
                piece = result_s.at[j, device]
                pltpu.make_async_copy(piece, piece, back_send.at[j, device]).wait()

    own_parts.wait()

    @pl.loop(0, count)
    def _(j):
        own_back(j).wait()
        own_text(j).wait()

    copy_own.wait_send()
    for side in range(2):
        @pl.when(core != side)
        def _():
            copy_og(0, side).wait_send()

    @pl.loop(1, images)
    def _(step):
        copy_io(step).wait_send()
        share_io(step).wait_send()
        copy_parts(step).wait_send()
        for side in range(2):
            copy_og(step, side).wait_send()
        source = (image + step) % images
        pltpu.make_async_copy(parts_ref.at[source], parts_ref.at[source], parts_recv.at[source]).wait()


def exchange(plan, *arrays):
    p = plan
    dma = pltpu.SemaphoreType.DMA
    anywhere = pl.BlockSpec(memory_space=pl.ANY)
    pick = up(p.heads, 8)
    wide = (p.total, p.depth)
    return pl.pallas_call(
        functools.partial(exchange_kernel, p),
        out_shape=(
            jax.ShapeDtypeStruct((p.heads, p.out_rows, p.depth), BF),
            jax.ShapeDtypeStruct((p.heads, p.out_text, p.depth), BF),
            jax.ShapeDtypeStruct((p.images, p.part, p.feature), BF),
        ),
        in_specs=[anywhere] * 13,
        out_specs=(anywhere,) * 3,
        scratch_shapes=[pltpu.VMEM((p.rows, p.feature), BF)] * 4
        + [
            pltpu.VMEM((p.rows, p.model), BF),
            pltpu.VMEM((p.heads, 1, p.rows), F32),
            pltpu.VMEM((p.heads, 1, p.text_rows), F32),
            pltpu.VMEM((p.most, p.out_text, p.depth), BF),
            pltpu.VMEM((p.model, p.feature), BF),
            pltpu.VMEM((5, p.text_rows, p.feature), BF),
            pltpu.VMEM((p.heads, p.rows, p.depth), BF),
            pltpu.VMEM((p.heads, p.rows, p.depth), BF),
            pltpu.VMEM((p.peers, p.stat_rows, p.rows), F32),
            pltpu.VMEM((p.most, *wide), BF),
            pltpu.VMEM((p.most, *wide), BF),
            pltpu.VMEM((p.peers, p.stat_rows, p.rows), F32),
            pltpu.VMEM((p.stat_rows, p.total - p.tokens), F32),
            pltpu.VMEM((pick, p.rows), F32),
            pltpu.VMEM((pick, p.text_rows), F32),
            pltpu.VMEM(wide, BF),
        ]
        + [pltpu.VMEM(wide, BF)] * 6
        + [
            pltpu.VMEM((p.depth, p.total), F32),
            pltpu.VMEM((p.most, p.peers, p.out_rows, p.depth), BF),
            pltpu.VMEM((2, p.chips, p.share_pad, p.rows), BF),
            pltpu.VMEM((p.chips, p.part, 2 * p.images * p.rows), BF),
            pltpu.VMEM((2 * p.images, p.rows, p.feature), BF),
            pltpu.VMEM((p.chips, p.part, p.feature), BF),
            pltpu.VMEM((p.chips // 2 + 1, p.part, p.feature), BF),
            pltpu.VMEM((p.chips // 2, p.chips // 2, p.part, p.feature), BF),
            dma((13,)), dma((2, p.most + 1)),
            dma((p.heads,)), dma((p.most,)),
            dma((p.heads,)), dma((p.most,)),
            dma((p.peers,)), dma((p.peers,)),
            dma((p.most, p.peers)), dma((p.heads,)),
            dma((p.heads, 3)), dma((p.heads,)),
            dma((2 * p.images,)), dma((2 * p.images,)),
            dma((p.images, 2)), dma((2 * p.images,)),
            dma((p.chips,)), dma((p.chips // 2 + 1,)), dma((p.chips // 2, p.chips // 2)),
            dma((p.images,)), dma((p.images,)),
        ],
        compiler_params=pltpu.CompilerParams(
            collective_id=0, has_side_effects=True, vmem_limit_bytes=60 << 20
        ),
    )(*arrays)


def finish_kernel(
    plan, back_in, tback_in, parts_in, dq_out, dk_out, dv_out, tdq_out, tdk_out, tdv_out, wg_out,
    back_ref, tback_ref, parts_ref, dq_ref, dk_ref, dv_ref, tdq_ref, tdk_ref, tdv_ref, wg_ref,
    load_sem, store_sem,
):
    p = plan
    width, rows, half, even = p.width, p.rows, p.text_half, p.text_even
    group = p.heads // p.finish_steps
    text_loads = [
        pltpu.make_async_copy(
            tback_in.at[pl.ds(step * group, group)], tback_ref.at[pl.ds(step * group, group)], load_sem.at[2 + step]
        )
        for step in range(p.finish_steps)
    ]
    load_parts = pltpu.make_async_copy(parts_in, parts_ref, load_sem.at[0])
    load_back = pltpu.make_async_copy(back_in, back_ref, load_sem.at[1])
    for load in (load_parts, load_back, *text_loads):
        load.start()
    stores = []

    def store(source, target):
        copy = pltpu.make_async_copy(source, target, store_sem.at[len(stores)])
        copy.start()
        stores.append(copy)

    load_parts.wait()
    for number in range(p.images):
        start = p.part_start(number)
        stop = min(start + p.part, p.share)
        wg_ref[start:stop, :] = parts_ref[number, 0 : stop - start, :].astype(F32)
    store(wg_ref, wg_out)

    def join(ref, pair, at, cols):
        return jnp.concatenate([ref[2 * pair, at, cols], ref[2 * pair + 1, at, cols]], axis=1)

    left, right = slice(0, width), slice(width, p.depth)
    load_back.wait()
    for pair in range(p.heads // 2):
        lanes = slice(pair * p.depth, (pair + 1) * p.depth)
        dq_ref[:, lanes] = join(back_ref, pair, slice(0, rows), left)
        dk_ref[:, lanes] = join(back_ref, pair, slice(0, rows), right)
        dv_ref[0 : rows // 2, lanes] = join(back_ref, pair, slice(rows, p.out_rows), left)
        dv_ref[rows // 2 : rows, lanes] = join(back_ref, pair, slice(rows, p.out_rows), right)
    store(dq_ref, dq_out)
    store(dk_ref, dk_out)
    store(dv_ref, dv_out)
    for step in range(p.finish_steps):
        text_loads[step].wait()
        for pair in range(step * group // 2, (step + 1) * group // 2):
            lanes = slice(pair * p.depth, (pair + 1) * p.depth)
            tdq_ref[:, lanes] = join(tback_ref, pair, slice(0, p.text_rows), left)
            tdk_ref[:, lanes] = join(tback_ref, pair, slice(0, p.text_rows), right)
            tdv_ref[0:half, lanes] = join(tback_ref, pair, slice(even, even + half), left)
            tdv_ref[half : p.text_rows, lanes] = join(tback_ref, pair, slice(even, even + p.text_rows - half), right)
        lanes = slice(step * group * width, (step + 1) * group * width)
        for source, target in ((tdq_ref, tdq_out), (tdk_ref, tdk_out), (tdv_ref, tdv_out)):
            store(source.at[:, lanes], target.at[:, lanes])
    for copy in stores:
        copy.wait()


def finish(plan, back, tback, parts):
    p = plan
    anywhere = pl.BlockSpec(memory_space=pl.ANY)
    token = jax.ShapeDtypeStruct((p.rows, p.feature), BF)
    text = jax.ShapeDtypeStruct((p.text_rows, p.feature), BF)
    outs = (token,) * 3 + (text,) * 3 + (jax.ShapeDtypeStruct((p.share, p.feature), F32),)
    return pl.pallas_call(
        functools.partial(finish_kernel, p),
        out_shape=outs,
        in_specs=[anywhere] * 3,
        out_specs=(anywhere,) * 7,
        scratch_shapes=[pltpu.VMEM(value.shape, value.dtype) for value in (back, tback, parts, *outs)]
        + [
            pltpu.SemaphoreType.DMA((2 + p.finish_steps,)),
            pltpu.SemaphoreType.DMA((4 + 3 * p.finish_steps,)),
        ],
        compiler_params=pltpu.CompilerParams(vmem_limit_bytes=60 << 20),
    )(back, tback, parts)


def shards(
    image_query,
    image_key,
    image_value,
    image_output,
    output_grad,
    image_logsum,
    text_query,
    text_key,
    text_value,
    text_output,
    text_grad,
    text_logsum,
    out_weight,
):
    plan = Plan(
        lax.axis_size("seq"),
        lax.axis_size("img"),
        image_query.shape[1],
        text_query.shape[1],
        output_grad.shape[2],
        image_query.shape[2],
        image_logsum.shape[2],
    )
    results = exchange(
        plan,
        image_query[0], image_key[0], image_value[0], image_output[0], output_grad[0], image_logsum.transpose(2, 0, 1),
        text_query[0], text_key[0], text_value[0], text_output[0], text_grad[0], text_logsum.transpose(2, 0, 1),
        out_weight,
    )
    *grads, weight_grad = finish(plan, *results)
    return (*(grad[None] for grad in grads), weight_grad)


def solution(mesh):
    token = P("img", "seq", None)
    text = P("img", None, None)
    return jax.shard_map(
        shards,
        mesh=mesh,
        in_specs=(token,) * 6 + (text,) * 6 + (P(),),
        out_specs=(token,) * 3 + (text,) * 3 + (P("seq", None),),
        check_vma=False,
    )
```

```python
import functools

import jax
import jax.numpy as jnp
from jax import lax
from jax.experimental import pallas as pl
from jax.experimental.pallas import tpu as pltpu
from jax.sharding import PartitionSpec as P

LANES = 128
SUB = 16
MESH = pl.DeviceIdType.MESH
NN = (((1,), (0,)), ((), ()))
NT = (((1,), (1,)), ((), ()))
TN = (((0,), (0,)), ((), ()))
BF = jnp.bfloat16
F32 = jnp.float32


def up(value, step):
    return -(-value // step) * step


class Plan:
    def __init__(self, peers, images, rows, text_rows, model, feature, heads):
        self.peers, self.images, self.rows = peers, images, rows
        self.text_rows, self.model, self.feature, self.heads = text_rows, model, feature, heads
        self.chips = peers // 2
        self.width = feature // heads
        self.depth = 2 * self.width
        self.most = -(-heads // peers)
        self.stat_rows = up(2 * self.most, 8)
        self.tokens = peers * rows
        self.total = self.tokens + up(text_rows, LANES)
        self.key_block = self.total // 8
        self.text_even = up(text_rows, SUB)
        self.text_half = up(self.text_even // 2, SUB)
        self.out_rows = rows + rows // 2
        self.out_text = self.text_even + self.text_half
        self.share = model // peers
        self.finish_steps = next(n for n in (5, 4, 3, 2, 1) if heads % (2 * n) == 0)
        self.share_pad = up(self.share, SUB)
        self.part = up(-(-self.share_pad // images), SUB)

    def first(self, device):
        return device * self.heads // self.peers

    def part_start(self, image):
        if isinstance(image, int):
            return min(image * self.part, self.share_pad - self.part)
        return pl.multiple_of(jnp.minimum(image * self.part, self.share_pad - self.part), SUB)


def exchange_kernel(
    plan,
    q_in, k_in, v_in, o_in, og_in_ref, ls_in,
    tq_ref, tk_ref, tv_ref, to_ref, tg_ref, tls_in, w_ref,
    back_ref, tback_ref, parts_ref,
    q_ref, k_ref, v_ref, o_ref, og_ref, ls_ref, tls_ref, text_s, w_s, txt_s, x_out, st_out, x_in, st_in, st_text, dots_s, tdots_s, stat_s,
    q_s, k_s, v_s, g_s, dk_s, dv_s, dq_s, result_s, ogt_s, og_in, io_in, sums_out, sums_in, gate_in,
    local_sem, own_sem, x_send, x_recv, st_send, st_recv, back_send, back_recv,
    text_send, text_recv, io_send, io_recv, og_send, og_recv, sums_send, sums_recv, gate_recv,
    parts_send, parts_recv,
):
    p = plan
    peers, images, rows, width, depth, chips = p.peers, p.images, p.rows, p.width, p.depth, p.chips
    scaling = width ** (-0.5)
    me = lax.axis_index("seq")
    image = lax.axis_index("img")
    chip, core = me // 2, me % 2
    first = p.first(me)
    count = p.first(me + 1) - first
    slot = image * 2 + core
    my_rows = pl.ds(pl.multiple_of(me * rows, rows), rows)

    def remote(source, target, send, recv, device):
        return pltpu.make_async_remote_copy(
            src_ref=source, dst_ref=target, send_sem=send, recv_sem=recv,
            device_id=device, device_id_type=MESH,
        )

    barrier = pltpu.get_barrier_semaphore()

    @pl.loop(1, peers)
    def _(step):
        pl.semaphore_signal(barrier, inc=1, device_id=(image, (me + step) % peers), device_id_type=MESH)

    @pl.loop(1, images)
    def _(step):
        for side in range(2):
            pl.semaphore_signal(
                barrier, inc=1, device_id=((image + step) % images, chip * 2 + side), device_id_type=MESH
            )

    pairs = {
        "q": (q_in, q_ref), "k": (k_in, k_ref), "o": (o_in, o_ref), "og": (og_in_ref, og_ref), "w": (w_ref, w_s),
        "v": (v_in, v_ref), "ls": (ls_in, ls_ref), "tls": (tls_in, tls_ref),
    }
    loads = {}
    for number, (name, (source, target)) in enumerate(pairs.items()):
        loads[name] = pltpu.make_async_copy(source, target, local_sem.at[number])
        loads[name].start()
    for number, source in enumerate((tq_ref, tk_ref, tv_ref, tg_ref, to_ref)):
        pltpu.make_async_copy(source, txt_s.at[number], local_sem.at[len(pairs)]).start()

    def wait_bytes(ref, sem):
        pltpu.make_async_copy(ref, ref, sem).wait()

    loads["q"].wait()
    loads["k"].wait()

    for head in range(p.heads):
        cols = slice(head * width, (head + 1) * width)
        x_out[head, 0] = jnp.concatenate([q_ref[:, cols] * jnp.asarray(scaling, BF), k_ref[:, cols]], axis=1)

    pl.semaphore_wait(barrier, peers - 1 + 2 * (images - 1))

    def targets(j, action):
        @pl.loop(0, peers)
        def _(step):
            device = (me + peers // 2 + step) % peers
            head = p.first(device) + j

            @pl.when((device != me) & (head < p.first(device + 1)))
            def _():
                action(device, head)

    def copy_x(j, part):
        if j == 0:
            return lambda device, head: remote(
                x_out.at[head, part], x_in.at[j, part, my_rows], x_send.at[part], x_recv.at[part], (image, device)
            )
        return lambda device, head: remote(
            x_out.at[head], x_in.at[j, :, my_rows], x_send.at[2], x_recv.at[1 + j], (image, device)
        )

    def copy_st(device):
        return remote(st_out.at[device], st_in.at[me], st_send.at[0], st_recv.at[0], (image, device))

    targets(0, lambda device, head: copy_x(0, 0)(device, head).start())

    loads["o"].wait()
    loads["og"].wait()

    def copy_io(step):
        return remote(
            o_ref, io_in.at[slot], io_send.at[0], io_recv.at[0], ((image + step) % images, me)
        )

    def share_io(step):
        source = ((image + step) % images) * 2 + core
        return remote(
            io_in.at[source], io_in.at[source], io_send.at[0], io_recv.at[1],
            (image, chip * 2 + 1 - core),
        )

    copy_own = remote(
        o_ref, io_in.at[slot], io_send.at[0], io_recv.at[1], (image, chip * 2 + 1 - core)
    )

    @pl.loop(1, images)
    def _(step):
        copy_io(step).start()

    copy_own.start()

    for number in range(-(-p.model // LANES)):
        lanes = slice(number * LANES, (number + 1) * LANES)
        dq_s[:, 0:rows] = jnp.zeros((LANES, rows), F32) + og_ref[:, lanes].astype(F32).T
        turned = dq_s[:, 0:rows]
        for device in range(peers):
            low = max(number * LANES, device * p.share)
            high = min((number + 1) * LANES, (device + 1) * p.share)
            if low < high:
                ogt_s[device % 2, device // 2, low - device * p.share : high - device * p.share, :] = turned[
                    low - number * LANES : high - number * LANES
                ].astype(BF)

    def copy_og(step, side):
        other = (image + step) % images
        return remote(
            ogt_s.at[side, :, pl.ds(p.part_start(other), p.part)],
            og_in.at[:, :, pl.ds(pl.multiple_of(slot * rows, rows), rows)],
            og_send.at[0],
            og_recv.at[0],
            (other, chip * 2 + side),
        )

    @pl.loop(1, images)
    def _(step):
        for side in range(2):
            copy_og(step, side).start()

    for side in range(2):
        @pl.when(core != side)
        def _():
            copy_og(0, side).start()

    og_in[:, :, pl.ds(pl.multiple_of(slot * rows, rows), rows)] = ogt_s[
        core, :, pl.ds(p.part_start(image), p.part)
    ]
    io_in[slot] = o_ref[...]

    loads["w"].wait()

    @pl.loop(0, p.feature // 256)
    def _(step):
        lanes = pl.ds(pl.multiple_of(step * 256, 256), 256)
        g_cols = jnp.dot(og_ref[...], w_s[:, lanes], preferred_element_type=F32).astype(BF)
        per = 256 // width
        for number in range(per):
            head = step * per + number
            x_out[head, 1, :, 0:width] = g_cols[:, number * width : (number + 1) * width]

    pick_rows = up(p.heads, 8)
    tag = lax.broadcasted_iota(jnp.int32, (pick_rows, p.feature), 0)
    lane_at = lax.broadcasted_iota(jnp.int32, (pick_rows, p.feature), 1)
    picker = jnp.where((lane_at >= tag * width) & (lane_at < (tag + 1) * width), 1.0, 0.0).astype(F32)

    def row_dots(grads, outputs):
        product = grads.astype(F32) * outputs.astype(F32)
        return lax.dot_general(
            picker, product, NT, precision=lax.Precision.HIGHEST, preferred_element_type=F32
        )

    gathered = jnp.concatenate([x_out[head, 1, :, 0:width] for head in range(p.heads)], axis=1)
    dots_s[...] = row_dots(gathered, o_ref[...])
    loads["v"].wait()
    loads["ls"].wait()
    for head in range(p.heads):
        x_out[head, 1, :, width:depth] = v_ref[:, head * width : (head + 1) * width]
    st_out[...] = jnp.zeros_like(st_out)
    for device in range(peers):
        for j in range(p.first(device + 1) - p.first(device)):
            head = p.first(device) + j
            st_out[device, 2 * j : 2 * j + 1, :] = -ls_ref[head]
            st_out[device, 2 * j + 1 : 2 * j + 2, :] = -dots_s[head : head + 1, :]

    @pl.loop(0, peers)
    def _(step):
        device = (me + peers // 2 + step) % peers

        @pl.when(device != me)
        def _():
            copy_st(device).start()

    targets(0, lambda device, head: copy_x(0, 1)(device, head).start())
    for j in range(1, p.most):
        targets(j, lambda device, head: copy_x(j, 0)(device, head).start())

    loads["tls"].wait()
    wait_bytes(txt_s, local_sem.at[len(pairs)])
    tdots_s[...] = row_dots(txt_s[3], txt_s[4])
    st_text[...] = jnp.zeros_like(st_text)
    text_at = slice(p.tokens, p.tokens + p.text_rows)
    pad_at = slice(p.tokens + p.text_rows // SUB * SUB, p.total)

    @pl.loop(0, count)
    def _(j):
        head = first + j
        tile = pl.ds(pl.multiple_of(head // 2 * depth, depth), depth)
        odd = head % 2 == 1

        def text_cols(number):
            value = txt_s[number, :, tile]
            return jnp.where(odd, value[:, width:], value[:, :width])

        x_in[j, 0, my_rows] = x_out[head, 0]
        x_in[j, 1, my_rows] = x_out[head, 1]
        x_in[j, 0, pad_at] = jnp.zeros((p.total - pad_at.start, depth), BF)
        x_in[j, 1, pad_at] = jnp.zeros((p.total - pad_at.start, depth), BF)
        x_in[j, 0, text_at] = jnp.concatenate([text_cols(0) * jnp.asarray(scaling, BF), text_cols(1)], axis=1)
        x_in[j, 1, text_at] = jnp.concatenate([text_cols(3), text_cols(2)], axis=1)
        st_text[pl.ds(2 * j, 1), 0 : p.text_rows] = -tls_ref[head]
        st_text[pl.ds(2 * j + 1, 1), 0 : p.text_rows] = -tdots_s[pl.ds(head, 1), :]

    def stats_tile(value):
        terms = []
        for _ in range(3):
            term = value.astype(BF).astype(F32)
            terms.append(term)
            value = value - term
        used = width + 3 * p.stat_rows
        return jnp.concatenate(
            [jnp.zeros((width, LANES), F32), *terms, jnp.zeros((depth - used, LANES), F32)], axis=0
        ).T.astype(BF)

    for number in range((p.total - p.tokens) // LANES):
        stat_s[p.tokens + number * LANES : p.tokens + (number + 1) * LANES, :] = stats_tile(
            st_text[:, number * LANES : (number + 1) * LANES]
        )

    st_in[me] = st_out[me]

    wait_bytes(st_in.at[pl.ds(0, peers - 1)], st_recv.at[0])

    @pl.loop(0, peers)
    def _(source):
        stat_s[pl.ds(pl.multiple_of(source * rows, rows), rows), :] = stats_tile(st_in[source])

    lane = lax.broadcasted_iota(jnp.int32, (p.total, depth), 1)

    def ones(start):
        inside = (lane == width + start)
        for number in range(1, 3):
            inside = inside | (lane == width + start + number * p.stat_rows)
        return jnp.where(inside, 1.0, 0.0).astype(BF)[:, width:]

    far = pl.ds(0, (peers - 1) * rows)

    others = chips * p.most

    def text_slot(head, owner):
        return owner // 2 * p.most + head - p.first(owner)

    def send_text(source, head, owner, upward, downward):
        def send(way, recv, device):
            remote(source, tback_ref.at[head], text_send.at[way], text_recv.at[recv], (image, device)).start()

        @pl.when(upward & (chip + 1 < chips))
        def _():
            send(0, text_slot(head, owner), me + 2)

        @pl.when(downward & (chip > 0))
        def _():
            send(1, text_slot(head, owner), me - 2)

        send(2, others, chip * 2 + 1 - core)

    def own_back(j):
        return pltpu.make_async_copy(result_s.at[j, me], back_ref.at[first + j], own_sem.at[0])

    def send_back(j):
        own_back(j).start()

        @pl.loop(0, peers)
        def _(step):
            block = (me + peers // 2 + step) % peers

            @pl.when(block != me)
            def _():
                remote(
                    result_s.at[j, block], back_ref.at[first + j], back_send.at[0], back_recv.at[0],
                    (image, block),
                ).start()

    def own_text(j):
        return pltpu.make_async_copy(text_s.at[j], tback_ref.at[first + j], own_sem.at[1])

    half_chips = chips // 2
    side, seat = chip // half_chips, chip % half_chips
    gate = half_chips - 1 + side
    near, beyond = side * half_chips, (1 - side) * half_chips
    edge = chip != gate

    def send_sum(number, target, recv, device):
        remote(
            sums_out.at[number], target, sums_send.at[0], recv, (image, device * 2 + core)
        ).start()

    def send_terms():
        for number in range(half_chips):
            @pl.when(edge)
            def _():
                send_sum(beyond + number, gate_in.at[seat, number], gate_recv.at[0], gate)

        for number in range(half_chips):
            @pl.when(number != seat)
            def _():
                send_sum(near + number, sums_in.at[seat], sums_recv.at[0], near + number)

    def pass_sums():
        @pl.when(chip == gate)
        def _():
            if half_chips > 1:
                wait_bytes(gate_in.at[pl.ds(0, half_chips - 1)], gate_recv.at[0])
            for number in range(half_chips):
                @pl.loop(1, half_chips)
                def _(step):
                    source = (seat + step) % half_chips

                    @pl.loop(0, p.feature // 256)
                    def _(step):
                        lanes = pl.ds(pl.multiple_of(step * 256, 256), 256)
                        total = sums_out[beyond + number, :, lanes].astype(F32)
                        total += gate_in[source, number, :, lanes].astype(F32)
                        sums_out[beyond + number, :, lanes] = total.astype(BF)

                send_sum(beyond + number, sums_in.at[half_chips], sums_recv.at[0], beyond + number)

    def pass_text(hop, low, high, inward=(True, False)):
        for upward in (True, False):
            source = chip - hop if upward else chip + hop
            inner = side == (0 if upward else 1)
            wanted = {(True,): inner, (False,): ~inner}.get(inward, True)

            @pl.when((source >= 0) & (source < chips) & wanted)
            def _():
                owner = source * 2 + core
                start, stop = p.first(owner), p.first(owner + 1)

                @pl.loop(start + low, jnp.minimum(stop, start + high))
                def _(head):
                    wait_bytes(tback_ref.at[head], text_recv.at[text_slot(head, owner)])
                    send_text(tback_ref.at[head], head, owner, upward, not upward)

    @pl.loop(0, count)
    def _(j):
        head = first + j
        @pl.when(j == 0)
        def _():
            for part in range(2):
                wait_bytes(x_in.at[0, part, far], x_recv.at[part])

        @pl.when(j > 0)
        def _():
            wait_bytes(x_in.at[j, :, far], x_recv.at[1 + j])

        both = x_in[j, 0]
        q_s[...] = jnp.where(lane < width, both, stat_s[...])
        k_s[...] = jnp.concatenate([both[:, width:], ones(2 * j)], axis=1)
        both = x_in[j, 1]
        g_s[...] = jnp.where(lane < width, both, stat_s[...])
        v_s[...] = jnp.concatenate([both[:, width:], ones(2 * j + 1)], axis=1)
        dq_s[...] = jnp.zeros_like(dq_s)

        @pl.loop(0, p.total // p.key_block)
        def _(step):
            at = pl.ds(pl.multiple_of(step * p.key_block, p.key_block), p.key_block)
            keys = k_s[at, :]
            scores = lax.dot_general(keys, q_s[...], NT, preferred_element_type=F32)
            weights = jnp.exp(scores)
            grads = lax.dot_general(v_s[at, :], g_s[...], NT, preferred_element_type=F32)
            low = (weights * grads).astype(BF)
            dv_s[at, :] = jnp.dot(weights.astype(BF), g_s[...], preferred_element_type=F32).astype(BF)
            dk_s[at, :] = jnp.dot(low, q_s[...], preferred_element_type=F32).astype(BF)
            dq_s[...] += lax.dot_general(keys, low, TN, preferred_element_type=F32)

        dq = (dq_s[:, p.tokens : p.total].T * scaling).astype(BF)
        even, half = p.text_even, p.text_half
        text_s[j, 0:even] = jnp.concatenate(
            [dq[:even, :width], dk_s[p.tokens : p.tokens + even, :width]], axis=1
        )
        text_s[j, even : even + half] = jnp.concatenate(
            [dv_s[p.tokens : p.tokens + half, :width], dv_s[p.tokens + half : p.tokens + 2 * half, :width]],
            axis=1,
        )
        own_text(j).start()
        send_text(text_s.at[j], head, me, True, True)

        @pl.when(j == 0)
        def _():
            if images > 1:
                wait_bytes(io_in.at[pl.ds(0, images - 1)], io_recv.at[0])

            @pl.loop(1, images)
            def _(step):
                share_io(step).start()

        @pl.when(j == 0)
        def _():
            wait_bytes(io_in.at[pl.ds(0, images)], io_recv.at[1])
            wait_bytes(og_in.at[:, :, pl.ds(0, (2 * images - 1) * rows)], og_recv.at[0])

            @pl.loop(0, p.feature // 256)
            def _(step):
                lanes = pl.ds(pl.multiple_of(step * 256, 256), 256)
                for number in range(chips):
                    total = jnp.zeros((p.part, 256), F32)
                    for source in range(2 * images):
                        total += jnp.dot(
                            og_in[number, :, source * rows : (source + 1) * rows],
                            io_in[source, :, lanes],
                            preferred_element_type=F32,
                        )
                    sums_out[number, :, lanes] = total.astype(BF)

            send_terms()

        @pl.loop(0, peers)
        def _(block):
            base = pl.multiple_of(block * rows, rows)
            dq = (dq_s[:, pl.ds(base, rows)].T * scaling).astype(BF)
            top = jnp.concatenate([dq[:, :width], dk_s[pl.ds(base, rows), :width]], axis=1)
            dv = dv_s[pl.ds(base, rows), :width]
            bottom = jnp.concatenate([dv[: rows // 2], dv[rows // 2 :]], axis=1)
            result_s[j, block, 0:rows] = top
            result_s[j, block, rows : p.out_rows] = bottom

        @pl.when(j == 0)
        def _():
            pass_text(1, 0, 1)

        @pl.when(j == jnp.minimum(1, count - 1))
        def _():
            pass_sums()

        @pl.when(j == jnp.where(edge, jnp.minimum(1, count - 1), 0))
        def _():
            send_back(0)


    pass_text(1, 1, p.most, (True,))

    @pl.loop(1, count)
    def _(j):
        send_back(j)

    pass_text(1, 1, 2, (False,))
    if chips > 2:
        pass_text(2, 0, 1)
    pass_text(1, 2, p.most, (False,))

    wait_bytes(sums_in.at[pl.ds(0, half_chips)], sums_recv.at[0])

    @pl.loop(0, half_chips + 1)
    def _(source):
        @pl.when(source != seat)
        def _():
            @pl.loop(0, p.feature // 256)
            def _(step):
                lanes = pl.ds(pl.multiple_of(step * 256, 256), 256)
                total = sums_out[chip, :, lanes].astype(F32) + sums_in[source, :, lanes].astype(F32)
                sums_out[chip, :, lanes] = total.astype(BF)

    own_parts = pltpu.make_async_copy(sums_out.at[chip], parts_ref.at[image], own_sem.at[2])
    own_parts.start()

    def copy_parts(step):
        return remote(
            sums_out.at[chip], parts_ref.at[image], parts_send.at[0], parts_recv.at[0],
            ((image + step) % images, me),
        )

    @pl.loop(1, images)
    def _(step):
        copy_parts(step).start()

    if chips > 2:
        pass_text(2, 1, p.most)
    for hop in range(3, chips):
        pass_text(hop, 0, p.most)

    own_parts.wait()
    if images > 1:
        wait_bytes(parts_ref.at[pl.ds(0, images - 1)], parts_recv.at[0])
        wait_bytes(parts_ref.at[pl.ds(0, images - 1)], parts_send.at[0])
    wait_bytes(io_in.at[pl.ds(0, 2 * images - 1)], io_send.at[0])
    wait_bytes(og_in.at[:, :, pl.ds(0, (2 * images - 1) * rows)], og_send.at[0])
    wait_bytes(st_in.at[pl.ds(0, peers - 1)], st_send.at[0])
    if chips > 1:
        wait_bytes(sums_out.at[pl.ds(0, chips - 1)], sums_send.at[0])

    def heads_of(number, side):
        return p.first(number * 2 + side + 1) - p.first(number * 2 + side)

    for device in range(peers):
        here, at = device // 2, device % 2
        mine = heads_of(here, at)
        same = [heads_of(number, at) for number in range(chips)]
        upward = sum(same[: here + 1]) if here + 1 < chips else 0
        downward = sum(same[here:]) if here > 0 else 0
        partner = p.heads - sum(same)

        @pl.when(me == device)
        def _():
            wait_bytes(back_ref.at[pl.ds(0, mine)], own_sem.at[0])
            wait_bytes(tback_ref.at[pl.ds(0, mine)], own_sem.at[1])
            for part in range(2):
                wait_bytes(x_out.at[pl.ds(0, peers - 1), part], x_send.at[part])
            if p.heads - peers > mine - 1:
                wait_bytes(x_out.at[pl.ds(0, p.heads - peers - mine + 1)], x_send.at[2])
            wait_bytes(result_s.at[pl.ds(0, mine), pl.ds(0, peers - 1)], back_send.at[0])
            wait_bytes(back_ref.at[pl.ds(0, p.heads - mine)], back_recv.at[0])
            for way, blocks in enumerate((upward, downward, sum(same))):
                if blocks:
                    wait_bytes(tback_ref.at[pl.ds(0, blocks)], text_send.at[way])
            wait_bytes(tback_ref.at[pl.ds(0, partner)], text_recv.at[others])


def exchange(plan, *arrays):
    p = plan
    dma = pltpu.SemaphoreType.DMA
    anywhere = pl.BlockSpec(memory_space=pl.ANY)
    pick = up(p.heads, 8)
    wide = (p.total, p.depth)
    return pl.pallas_call(
        functools.partial(exchange_kernel, p),
        out_shape=(
            jax.ShapeDtypeStruct((p.heads, p.out_rows, p.depth), BF),
            jax.ShapeDtypeStruct((p.heads, p.out_text, p.depth), BF),
            jax.ShapeDtypeStruct((p.images, p.part, p.feature), BF),
        ),
        in_specs=[anywhere] * 13,
        out_specs=(anywhere,) * 3,
        scratch_shapes=[pltpu.VMEM((p.rows, p.feature), BF)] * 4
        + [
            pltpu.VMEM((p.rows, p.model), BF),
            pltpu.VMEM((p.heads, 1, p.rows), F32),
            pltpu.VMEM((p.heads, 1, p.text_rows), F32),
            pltpu.VMEM((p.most, p.out_text, p.depth), BF),
            pltpu.VMEM((p.model, p.feature), BF),
            pltpu.VMEM((5, p.text_rows, p.feature), BF),
            pltpu.VMEM((p.heads, 2, p.rows, p.depth), BF),
            pltpu.VMEM((p.peers, p.stat_rows, p.rows), F32),
            pltpu.VMEM((p.most, 2, *wide), BF),
            pltpu.VMEM((p.peers, p.stat_rows, p.rows), F32),
            pltpu.VMEM((p.stat_rows, p.total - p.tokens), F32),
            pltpu.VMEM((pick, p.rows), F32),
            pltpu.VMEM((pick, p.text_rows), F32),
            pltpu.VMEM(wide, BF),
        ]
        + [pltpu.VMEM(wide, BF)] * 6
        + [
            pltpu.VMEM((p.depth, p.total), F32),
            pltpu.VMEM((p.most, p.peers, p.out_rows, p.depth), BF),
            pltpu.VMEM((2, p.chips, p.share_pad, p.rows), BF),
            pltpu.VMEM((p.chips, p.part, 2 * p.images * p.rows), BF),
            pltpu.VMEM((2 * p.images, p.rows, p.feature), BF),
            pltpu.VMEM((p.chips, p.part, p.feature), BF),
            pltpu.VMEM((p.chips // 2 + 1, p.part, p.feature), BF),
            pltpu.VMEM((p.chips // 2, p.chips // 2, p.part, p.feature), BF),
            dma((9,)), dma((3,)),
            dma((3,)), dma((p.most + 1,)),
            dma((1,)), dma((1,)),
            dma((1,)), dma((1,)),
            dma((3,)), dma((p.chips * p.most + 1,)),
            dma((1,)), dma((2,)),
            dma((1,)), dma((1,)),
            dma((1,)), dma((1,)), dma((1,)),
            dma((1,)), dma((1,)),
        ],
        compiler_params=pltpu.CompilerParams(
            collective_id=0, has_side_effects=True, vmem_limit_bytes=60 << 20
        ),
    )(*arrays)


def finish_kernel(
    plan, back_in, tback_in, parts_in, dq_out, dk_out, dv_out, tdq_out, tdk_out, tdv_out, wg_out,
    back_ref, tback_ref, parts_ref, dq_ref, dk_ref, dv_ref, tdq_ref, tdk_ref, tdv_ref, wg_ref,
    load_sem, store_sem,
):
    p = plan
    width, rows, half, even = p.width, p.rows, p.text_half, p.text_even
    group = p.heads // p.finish_steps
    text_loads = [
        pltpu.make_async_copy(
            tback_in.at[pl.ds(step * group, group)], tback_ref.at[pl.ds(step * group, group)], load_sem.at[2 + step]
        )
        for step in range(p.finish_steps)
    ]
    load_parts = pltpu.make_async_copy(parts_in, parts_ref, load_sem.at[0])
    load_back = pltpu.make_async_copy(back_in, back_ref, load_sem.at[1])
    for load in (load_parts, load_back, *text_loads):
        load.start()
    stores = []

    def store(source, target):
        copy = pltpu.make_async_copy(source, target, store_sem.at[len(stores)])
        copy.start()
        stores.append(copy)

    whole = [
        pltpu.make_async_copy(source, target, store_sem.at[4 + number])
        for number, (source, target) in enumerate(((tdq_ref, tdq_out), (tdk_ref, tdk_out), (tdv_ref, tdv_out)))
    ]

    load_parts.wait()
    for number in range(p.images):
        start = p.part_start(number)
        stop = min(start + p.part, p.share)
        wg_ref[start:stop, :] = parts_ref[number, 0 : stop - start, :].astype(F32)
    store(wg_ref, wg_out)

    def join(ref, pair, at, cols):
        return jnp.concatenate([ref[2 * pair, at, cols], ref[2 * pair + 1, at, cols]], axis=1)

    left, right = slice(0, width), slice(width, p.depth)
    load_back.wait()
    for pair in range(p.heads // 2):
        lanes = slice(pair * p.depth, (pair + 1) * p.depth)
        dq_ref[:, lanes] = join(back_ref, pair, slice(0, rows), left)
        dk_ref[:, lanes] = join(back_ref, pair, slice(0, rows), right)
        dv_ref[0 : rows // 2, lanes] = join(back_ref, pair, slice(rows, p.out_rows), left)
        dv_ref[rows // 2 : rows, lanes] = join(back_ref, pair, slice(rows, p.out_rows), right)
    store(dq_ref, dq_out)
    store(dk_ref, dk_out)
    store(dv_ref, dv_out)
    for step in range(p.finish_steps):
        text_loads[step].wait()
        for pair in range(step * group // 2, (step + 1) * group // 2):
            lanes = slice(pair * p.depth, (pair + 1) * p.depth)
            tdq_ref[:, lanes] = join(tback_ref, pair, slice(0, p.text_rows), left)
            tdk_ref[:, lanes] = join(tback_ref, pair, slice(0, p.text_rows), right)
            tdv_ref[0:half, lanes] = join(tback_ref, pair, slice(even, even + half), left)
            tdv_ref[half : p.text_rows, lanes] = join(tback_ref, pair, slice(even, even + p.text_rows - half), right)
        lanes = slice(step * group * width, (step + 1) * group * width)
        for number, (source, target) in enumerate(((tdq_ref, tdq_out), (tdk_ref, tdk_out), (tdv_ref, tdv_out))):
            pltpu.make_async_copy(source.at[:, lanes], target.at[:, lanes], store_sem.at[4 + number]).start()
    for copy in (*stores, *whole):
        copy.wait()


def finish(plan, back, tback, parts):
    p = plan
    anywhere = pl.BlockSpec(memory_space=pl.ANY)
    token = jax.ShapeDtypeStruct((p.rows, p.feature), BF)
    text = jax.ShapeDtypeStruct((p.text_rows, p.feature), BF)
    outs = (token,) * 3 + (text,) * 3 + (jax.ShapeDtypeStruct((p.share, p.feature), F32),)
    return pl.pallas_call(
        functools.partial(finish_kernel, p),
        out_shape=outs,
        in_specs=[anywhere] * 3,
        out_specs=(anywhere,) * 7,
        scratch_shapes=[pltpu.VMEM(value.shape, value.dtype) for value in (back, tback, parts, *outs)]
        + [
            pltpu.SemaphoreType.DMA((2 + p.finish_steps,)),
            pltpu.SemaphoreType.DMA((7,)),
        ],
        compiler_params=pltpu.CompilerParams(vmem_limit_bytes=60 << 20),
    )(back, tback, parts)


def shards(
    image_query,
    image_key,
    image_value,
    image_output,
    output_grad,
    image_logsum,
    text_query,
    text_key,
    text_value,
    text_output,
    text_grad,
    text_logsum,
    out_weight,
):
    plan = Plan(
        lax.axis_size("seq"),
        lax.axis_size("img"),
        image_query.shape[1],
        text_query.shape[1],
        output_grad.shape[2],
        image_query.shape[2],
        image_logsum.shape[2],
    )
    results = exchange(
        plan,
        image_query[0], image_key[0], image_value[0], image_output[0], output_grad[0], image_logsum.transpose(2, 0, 1),
        text_query[0], text_key[0], text_value[0], text_output[0], text_grad[0], text_logsum.transpose(2, 0, 1),
        out_weight,
    )
    *grads, weight_grad = finish(plan, *results)
    return (*(grad[None] for grad in grads), weight_grad)


def solution(mesh):
    token = P("img", "seq", None)
    text = P("img", None, None)
    return jax.shard_map(
        shards,
        mesh=mesh,
        in_specs=(token,) * 6 + (text,) * 6 + (P(),),
        out_specs=(token,) * 3 + (text,) * 3 + (P("seq", None),),
        check_vma=False,
    )
```

```python
import functools

import jax
import jax.numpy as jnp
from jax import lax
from jax.experimental import pallas as pl
from jax.experimental.pallas import tpu as pltpu
from jax.sharding import PartitionSpec as P

LANES = 128
SUB = 16
MESH = pl.DeviceIdType.MESH
NN = (((1,), (0,)), ((), ()))
NT = (((1,), (1,)), ((), ()))
TN = (((0,), (0,)), ((), ()))
BF = jnp.bfloat16
F32 = jnp.float32


def up(value, step):
    return -(-value // step) * step


class Plan:
    def __init__(self, peers, images, rows, text_rows, model, feature, heads):
        self.peers, self.images, self.rows = peers, images, rows
        self.text_rows, self.model, self.feature, self.heads = text_rows, model, feature, heads
        self.chips = peers // 2
        self.width = feature // heads
        self.depth = 2 * self.width
        self.most = -(-heads // peers)
        self.stat_rows = up(2 * self.most, 8)
        self.tokens = peers * rows
        self.total = self.tokens + up(text_rows, LANES)
        self.key_block = self.total // 8
        self.text_even = up(text_rows, SUB)
        self.text_half = up(self.text_even // 2, SUB)
        self.out_rows = rows + rows // 2
        self.out_text = self.text_even + self.text_half
        self.share = model // peers
        self.finish_steps = next(n for n in (5, 4, 3, 2, 1) if heads % (2 * n) == 0)
        self.share_pad = up(self.share, SUB)
        self.part = up(-(-self.share_pad // images), SUB)

    def first(self, device):
        return device * self.heads // self.peers

    def part_start(self, image):
        if isinstance(image, int):
            return min(image * self.part, self.share_pad - self.part)
        return pl.multiple_of(jnp.minimum(image * self.part, self.share_pad - self.part), SUB)


def exchange_kernel(
    plan,
    q_in, k_in, v_in, o_in, og_in_ref, ls_in,
    tq_ref, tk_ref, tv_ref, to_ref, tg_ref, tls_in, w_ref,
    back_ref, tback_ref, parts_ref,
    q_ref, k_ref, v_ref, o_ref, og_ref, ls_ref, tls_ref, text_s, w_s, txt_s, x_out, st_out, x_in, st_in, st_text, dots_s, tdots_s, stat_s,
    q_s, k_s, v_s, g_s, dk_s, dv_s, dq_s, result_s, ogt_s, og_in, io_in, sums_out, sums_in, gate_in,
    local_sem, own_sem, x_send, x_recv, st_send, st_recv, back_send, back_recv,
    text_send, text_recv, io_send, io_recv, og_send, og_recv, sums_send, sums_recv, gate_recv,
    parts_send, parts_recv,
):
    p = plan
    peers, images, rows, width, depth, chips = p.peers, p.images, p.rows, p.width, p.depth, p.chips
    scaling = width ** (-0.5)
    me = lax.axis_index("seq")
    image = lax.axis_index("img")
    chip, core = me // 2, me % 2
    first = p.first(me)
    count = p.first(me + 1) - first
    slot = image * 2 + core
    my_rows = pl.ds(pl.multiple_of(me * rows, rows), rows)

    def remote(source, target, send, recv, device):
        return pltpu.make_async_remote_copy(
            src_ref=source, dst_ref=target, send_sem=send, recv_sem=recv,
            device_id=device, device_id_type=MESH,
        )

    barrier = pltpu.get_barrier_semaphore()

    @pl.loop(1, peers)
    def _(step):
        pl.semaphore_signal(barrier, inc=1, device_id=(image, (me + step) % peers), device_id_type=MESH)

    @pl.loop(1, images)
    def _(step):
        for side in range(2):
            pl.semaphore_signal(
                barrier, inc=1, device_id=((image + step) % images, chip * 2 + side), device_id_type=MESH
            )

    pairs = {
        "q": (q_in, q_ref), "k": (k_in, k_ref), "o": (o_in, o_ref), "og": (og_in_ref, og_ref), "w": (w_ref, w_s),
        "v": (v_in, v_ref), "ls": (ls_in, ls_ref), "tls": (tls_in, tls_ref),
    }
    loads = {}
    for number, (name, (source, target)) in enumerate(pairs.items()):
        loads[name] = pltpu.make_async_copy(source, target, local_sem.at[number])
        loads[name].start()
    for number, source in enumerate((tq_ref, tk_ref, tv_ref, tg_ref, to_ref)):
        pltpu.make_async_copy(source, txt_s.at[number], local_sem.at[len(pairs)]).start()

    def wait_bytes(ref, sem):
        pltpu.make_async_copy(ref, ref, sem).wait()

    loads["q"].wait()
    loads["k"].wait()

    for head in range(p.heads):
        cols = slice(head * width, (head + 1) * width)
        x_out[head, 0] = jnp.concatenate([q_ref[:, cols] * jnp.asarray(scaling, BF), k_ref[:, cols]], axis=1)

    pl.semaphore_wait(barrier, peers - 1 + 2 * (images - 1))

    def targets(j, action):
        @pl.loop(0, peers)
        def _(step):
            device = (me + peers // 2 + step) % peers
            head = p.first(device) + j

            @pl.when((device != me) & (head < p.first(device + 1)))
            def _():
                action(device, head)

    def copy_x(j, part):
        if j == 0:
            return lambda device, head: remote(
                x_out.at[head, part], x_in.at[j, part, my_rows], x_send.at[part], x_recv.at[part], (image, device)
            )
        return lambda device, head: remote(
            x_out.at[head], x_in.at[j, :, my_rows], x_send.at[2], x_recv.at[1 + j], (image, device)
        )

    def copy_st(device):
        return remote(st_out.at[device], st_in.at[me], st_send.at[0], st_recv.at[0], (image, device))

    targets(0, lambda device, head: copy_x(0, 0)(device, head).start())

    loads["o"].wait()
    loads["og"].wait()

    def copy_io(step):
        return remote(
            o_ref, io_in.at[slot], io_send.at[0], io_recv.at[0], ((image + step) % images, me)
        )

    def share_io(step):
        source = ((image + step) % images) * 2 + core
        return remote(
            io_in.at[source], io_in.at[source], io_send.at[0], io_recv.at[1],
            (image, chip * 2 + 1 - core),
        )

    copy_own = remote(
        o_ref, io_in.at[slot], io_send.at[0], io_recv.at[1], (image, chip * 2 + 1 - core)
    )

    @pl.loop(1, images)
    def _(step):
        copy_io(step).start()

    copy_own.start()

    for number in range(-(-p.model // LANES)):
        lanes = slice(number * LANES, (number + 1) * LANES)
        dq_s[:, 0:rows] = jnp.zeros((LANES, rows), F32) + og_ref[:, lanes].astype(F32).T
        turned = dq_s[:, 0:rows]
        for device in range(peers):
            low = max(number * LANES, device * p.share)
            high = min((number + 1) * LANES, (device + 1) * p.share)
            if low < high:
                ogt_s[device % 2, device // 2, low - device * p.share : high - device * p.share, :] = turned[
                    low - number * LANES : high - number * LANES
                ].astype(BF)

    def copy_og(step, side):
        other = (image + step) % images
        return remote(
            ogt_s.at[side, :, pl.ds(p.part_start(other), p.part)],
            og_in.at[:, :, pl.ds(pl.multiple_of(slot * rows, rows), rows)],
            og_send.at[0],
            og_recv.at[0],
            (other, chip * 2 + side),
        )

    @pl.loop(1, images)
    def _(step):
        for side in range(2):
            copy_og(step, side).start()

    for side in range(2):
        @pl.when(core != side)
        def _():
            copy_og(0, side).start()

    og_in[:, :, pl.ds(pl.multiple_of(slot * rows, rows), rows)] = ogt_s[
        core, :, pl.ds(p.part_start(image), p.part)
    ]
    io_in[slot] = o_ref[...]

    loads["w"].wait()

    @pl.loop(0, p.feature // 256)
    def _(step):
        lanes = pl.ds(pl.multiple_of(step * 256, 256), 256)
        g_cols = jnp.dot(og_ref[...], w_s[:, lanes], preferred_element_type=F32).astype(BF)
        per = 256 // width
        for number in range(per):
            head = step * per + number
            x_out[head, 1, :, 0:width] = g_cols[:, number * width : (number + 1) * width]

    pick_rows = up(p.heads, 8)
    tag = lax.broadcasted_iota(jnp.int32, (pick_rows, p.feature), 0)
    lane_at = lax.broadcasted_iota(jnp.int32, (pick_rows, p.feature), 1)
    picker = jnp.where((lane_at >= tag * width) & (lane_at < (tag + 1) * width), 1.0, 0.0).astype(F32)

    def row_dots(grads, outputs):
        product = grads.astype(F32) * outputs.astype(F32)
        return lax.dot_general(
            picker, product, NT, precision=lax.Precision.HIGHEST, preferred_element_type=F32
        )

    gathered = jnp.concatenate([x_out[head, 1, :, 0:width] for head in range(p.heads)], axis=1)
    dots_s[...] = row_dots(gathered, o_ref[...])
    loads["v"].wait()
    loads["ls"].wait()
    for head in range(p.heads):
        x_out[head, 1, :, width:depth] = v_ref[:, head * width : (head + 1) * width]
    st_out[...] = jnp.zeros_like(st_out)
    for device in range(peers):
        for j in range(p.first(device + 1) - p.first(device)):
            head = p.first(device) + j
            st_out[device, 2 * j : 2 * j + 1, :] = -ls_ref[head]
            st_out[device, 2 * j + 1 : 2 * j + 2, :] = -dots_s[head : head + 1, :]

    @pl.loop(0, peers)
    def _(step):
        device = (me + peers // 2 + step) % peers

        @pl.when(device != me)
        def _():
            copy_st(device).start()

    targets(0, lambda device, head: copy_x(0, 1)(device, head).start())
    for j in range(1, p.most):
        targets(j, lambda device, head: copy_x(j, 0)(device, head).start())

    loads["tls"].wait()
    wait_bytes(txt_s, local_sem.at[len(pairs)])
    tdots_s[...] = row_dots(txt_s[3], txt_s[4])
    st_text[...] = jnp.zeros_like(st_text)
    text_at = slice(p.tokens, p.tokens + p.text_rows)
    pad_at = slice(p.tokens + p.text_rows // SUB * SUB, p.total)

    @pl.loop(0, count)
    def _(j):
        head = first + j
        tile = pl.ds(pl.multiple_of(head // 2 * depth, depth), depth)
        odd = head % 2 == 1

        def text_cols(number):
            value = txt_s[number, :, tile]
            return jnp.where(odd, value[:, width:], value[:, :width])

        x_in[j, 0, my_rows] = x_out[head, 0]
        x_in[j, 1, my_rows] = x_out[head, 1]
        x_in[j, 0, pad_at] = jnp.zeros((p.total - pad_at.start, depth), BF)
        x_in[j, 1, pad_at] = jnp.zeros((p.total - pad_at.start, depth), BF)
        x_in[j, 0, text_at] = jnp.concatenate([text_cols(0) * jnp.asarray(scaling, BF), text_cols(1)], axis=1)
        x_in[j, 1, text_at] = jnp.concatenate([text_cols(3), text_cols(2)], axis=1)
        st_text[pl.ds(2 * j, 1), 0 : p.text_rows] = -tls_ref[head]
        st_text[pl.ds(2 * j + 1, 1), 0 : p.text_rows] = -tdots_s[pl.ds(head, 1), :]

    def stats_tile(value):
        terms = []
        for _ in range(3):
            term = value.astype(BF).astype(F32)
            terms.append(term)
            value = value - term
        used = width + 3 * p.stat_rows
        return jnp.concatenate(
            [jnp.zeros((width, LANES), F32), *terms, jnp.zeros((depth - used, LANES), F32)], axis=0
        ).T.astype(BF)

    for number in range((p.total - p.tokens) // LANES):
        stat_s[p.tokens + number * LANES : p.tokens + (number + 1) * LANES, :] = stats_tile(
            st_text[:, number * LANES : (number + 1) * LANES]
        )

    st_in[me] = st_out[me]

    wait_bytes(st_in.at[pl.ds(0, peers - 1)], st_recv.at[0])

    @pl.loop(0, peers)
    def _(source):
        stat_s[pl.ds(pl.multiple_of(source * rows, rows), rows), :] = stats_tile(st_in[source])

    lane = lax.broadcasted_iota(jnp.int32, (p.total, depth), 1)

    def ones(start):
        inside = (lane == width + start)
        for number in range(1, 3):
            inside = inside | (lane == width + start + number * p.stat_rows)
        return jnp.where(inside, 1.0, 0.0).astype(BF)[:, width:]

    far = pl.ds(0, (peers - 1) * rows)

    others = chips * p.most

    def text_slot(head, owner):
        return owner // 2 * p.most + head - p.first(owner)

    def send_text(source, head, owner, upward, downward):
        def send(way, recv, device):
            remote(source, tback_ref.at[head], text_send.at[way], text_recv.at[recv], (image, device)).start()

        @pl.when(upward & (chip + 1 < chips))
        def _():
            send(0, text_slot(head, owner), me + 2)

        @pl.when(downward & (chip > 0))
        def _():
            send(1, text_slot(head, owner), me - 2)

        send(2, others, chip * 2 + 1 - core)

    def own_back(j):
        return pltpu.make_async_copy(result_s.at[j, me], back_ref.at[first + j], own_sem.at[0])

    def send_back(j):
        own_back(j).start()

        @pl.loop(0, peers)
        def _(step):
            block = (me + peers // 2 + step) % peers

            @pl.when(block != me)
            def _():
                remote(
                    result_s.at[j, block], back_ref.at[first + j], back_send.at[0], back_recv.at[0],
                    (image, block),
                ).start()

    def own_text(j):
        return pltpu.make_async_copy(text_s.at[j], tback_ref.at[first + j], own_sem.at[1])

    half_chips = chips // 2
    side, seat = chip // half_chips, chip % half_chips
    gate = half_chips - 1 + side
    near, beyond = side * half_chips, (1 - side) * half_chips
    edge = chip != gate

    def send_sum(number, target, recv, device):
        remote(
            sums_out.at[number], target, sums_send.at[0], recv, (image, device * 2 + core)
        ).start()

    def send_terms():
        for number in range(half_chips):
            @pl.when(edge)
            def _():
                send_sum(beyond + number, gate_in.at[seat, number], gate_recv.at[0], gate)

        for number in range(half_chips):
            @pl.when(number != seat)
            def _():
                send_sum(near + number, sums_in.at[seat], sums_recv.at[0], near + number)

    def pass_sums():
        @pl.when(chip == gate)
        def _():
            if half_chips > 1:
                wait_bytes(gate_in.at[pl.ds(0, half_chips - 1)], gate_recv.at[0])
            for number in range(half_chips):
                @pl.loop(1, half_chips)
                def _(step):
                    source = (seat + step) % half_chips

                    @pl.loop(0, p.feature // 256)
                    def _(step):
                        lanes = pl.ds(pl.multiple_of(step * 256, 256), 256)
                        total = sums_out[beyond + number, :, lanes].astype(F32)
                        total += gate_in[source, number, :, lanes].astype(F32)
                        sums_out[beyond + number, :, lanes] = total.astype(BF)

                send_sum(beyond + number, sums_in.at[half_chips], sums_recv.at[0], beyond + number)

    def pass_text(hop, low, high, inward=(True, False)):
        for upward in (True, False):
            source = chip - hop if upward else chip + hop
            inner = side == (0 if upward else 1)
            wanted = {(True,): inner, (False,): ~inner}.get(inward, True)

            @pl.when((source >= 0) & (source < chips) & wanted)
            def _():
                owner = source * 2 + core
                start, stop = p.first(owner), p.first(owner + 1)

                @pl.loop(start + low, jnp.minimum(stop, start + high))
                def _(head):
                    wait_bytes(tback_ref.at[head], text_recv.at[text_slot(head, owner)])
                    send_text(tback_ref.at[head], head, owner, upward, not upward)

    @pl.loop(0, count)
    def _(j):
        head = first + j
        @pl.when(j == 0)
        def _():
            for part in range(2):
                wait_bytes(x_in.at[0, part, far], x_recv.at[part])

        @pl.when(j > 0)
        def _():
            wait_bytes(x_in.at[j, :, far], x_recv.at[1 + j])

        both = x_in[j, 0]
        q_s[...] = jnp.where(lane < width, both, stat_s[...])
        k_s[...] = jnp.concatenate([both[:, width:], ones(2 * j)], axis=1)
        both = x_in[j, 1]
        g_s[...] = jnp.where(lane < width, both, stat_s[...])
        v_s[...] = jnp.concatenate([both[:, width:], ones(2 * j + 1)], axis=1)
        dq_s[...] = jnp.zeros_like(dq_s)

        @pl.loop(0, p.total // p.key_block)
        def _(step):
            at = pl.ds(pl.multiple_of(step * p.key_block, p.key_block), p.key_block)
            keys = k_s[at, :]
            scores = lax.dot_general(keys, q_s[...], NT, preferred_element_type=F32)
            weights = jnp.exp(scores)
            grads = lax.dot_general(v_s[at, :], g_s[...], NT, preferred_element_type=F32)
            low = (weights * grads).astype(BF)
            dv_s[at, :] = jnp.dot(weights.astype(BF), g_s[...], preferred_element_type=F32).astype(BF)
            dk_s[at, :] = jnp.dot(low, q_s[...], preferred_element_type=F32).astype(BF)
            dq_s[...] += lax.dot_general(keys, low, TN, preferred_element_type=F32)

        dq = (dq_s[:, p.tokens : p.total].T * scaling).astype(BF)
        even, half = p.text_even, p.text_half
        text_s[j, 0:even] = jnp.concatenate(
            [dq[:even, :width], dk_s[p.tokens : p.tokens + even, :width]], axis=1
        )
        text_s[j, even : even + half] = jnp.concatenate(
            [dv_s[p.tokens : p.tokens + half, :width], dv_s[p.tokens + half : p.tokens + 2 * half, :width]],
            axis=1,
        )
        own_text(j).start()
        send_text(text_s.at[j], head, me, True, True)

        @pl.when(j == 0)
        def _():
            if images > 1:
                wait_bytes(io_in.at[pl.ds(0, images - 1)], io_recv.at[0])

            @pl.loop(1, images)
            def _(step):
                share_io(step).start()

        @pl.when(j == 0)
        def _():
            wait_bytes(io_in.at[pl.ds(0, images)], io_recv.at[1])
            wait_bytes(og_in.at[:, :, pl.ds(0, (2 * images - 1) * rows)], og_recv.at[0])

            @pl.loop(0, p.feature // 256)
            def _(step):
                lanes = pl.ds(pl.multiple_of(step * 256, 256), 256)
                for number in range(chips):
                    total = jnp.zeros((p.part, 256), F32)
                    for source in range(2 * images):
                        total += jnp.dot(
                            og_in[number, :, source * rows : (source + 1) * rows],
                            io_in[source, :, lanes],
                            preferred_element_type=F32,
                        )
                    sums_out[number, :, lanes] = total.astype(BF)

            send_terms()

        @pl.loop(0, peers)
        def _(block):
            base = pl.multiple_of(block * rows, rows)
            dq = (dq_s[:, pl.ds(base, rows)].T * scaling).astype(BF)
            top = jnp.concatenate([dq[:, :width], dk_s[pl.ds(base, rows), :width]], axis=1)
            dv = dv_s[pl.ds(base, rows), :width]
            bottom = jnp.concatenate([dv[: rows // 2], dv[rows // 2 :]], axis=1)
            result_s[j, block, 0:rows] = top
            result_s[j, block, rows : p.out_rows] = bottom

        @pl.when(j == 0)
        def _():
            pass_text(1, 0, 1)

        @pl.when(j == jnp.minimum(1, count - 1))
        def _():
            pass_sums()

        @pl.when(j == jnp.where(edge, jnp.minimum(1, count - 1), 0))
        def _():
            send_back(0)


    pass_text(1, 1, p.most, (True,))

    @pl.loop(1, count)
    def _(j):
        send_back(j)

    pass_text(1, 1, 2, (False,))
    if chips > 2:
        pass_text(2, 0, 1)
    pass_text(1, 2, p.most, (False,))

    wait_bytes(sums_in.at[pl.ds(0, half_chips)], sums_recv.at[0])

    @pl.loop(0, half_chips + 1)
    def _(source):
        @pl.when(source != seat)
        def _():
            @pl.loop(0, p.feature // 256)
            def _(step):
                lanes = pl.ds(pl.multiple_of(step * 256, 256), 256)
                total = sums_out[chip, :, lanes].astype(F32) + sums_in[source, :, lanes].astype(F32)
                sums_out[chip, :, lanes] = total.astype(BF)

    own_parts = pltpu.make_async_copy(sums_out.at[chip], parts_ref.at[image], own_sem.at[2])
    own_parts.start()

    def copy_parts(step):
        return remote(
            sums_out.at[chip], parts_ref.at[image], parts_send.at[0], parts_recv.at[0],
            ((image + step) % images, me),
        )

    @pl.loop(1, images)
    def _(step):
        copy_parts(step).start()

    if chips > 2:
        pass_text(2, 1, p.most)
    for hop in range(3, chips):
        pass_text(hop, 0, p.most)

    own_parts.wait()
    if images > 1:
        wait_bytes(parts_ref.at[pl.ds(0, images - 1)], parts_recv.at[0])
        wait_bytes(parts_ref.at[pl.ds(0, images - 1)], parts_send.at[0])
    wait_bytes(io_in.at[pl.ds(0, 2 * images - 1)], io_send.at[0])
    wait_bytes(og_in.at[:, :, pl.ds(0, (2 * images - 1) * rows)], og_send.at[0])
    wait_bytes(st_in.at[pl.ds(0, peers - 1)], st_send.at[0])
    if chips > 1:
        wait_bytes(sums_out.at[pl.ds(0, chips - 1)], sums_send.at[0])

    def heads_of(number, side):
        return p.first(number * 2 + side + 1) - p.first(number * 2 + side)

    for device in range(peers):
        here, at = device // 2, device % 2
        mine = heads_of(here, at)
        same = [heads_of(number, at) for number in range(chips)]
        upward = sum(same[: here + 1]) if here + 1 < chips else 0
        downward = sum(same[here:]) if here > 0 else 0
        partner = p.heads - sum(same)

        @pl.when(me == device)
        def _():
            wait_bytes(back_ref.at[pl.ds(0, mine)], own_sem.at[0])
            wait_bytes(tback_ref.at[pl.ds(0, mine)], own_sem.at[1])
            for part in range(2):
                wait_bytes(x_out.at[pl.ds(0, peers - 1), part], x_send.at[part])
            if p.heads - peers > mine - 1:
                wait_bytes(x_out.at[pl.ds(0, p.heads - peers - mine + 1)], x_send.at[2])
            wait_bytes(result_s.at[pl.ds(0, mine), pl.ds(0, peers - 1)], back_send.at[0])
            wait_bytes(back_ref.at[pl.ds(0, p.heads - mine)], back_recv.at[0])
            for way, blocks in enumerate((upward, downward, sum(same))):
                if blocks:
                    wait_bytes(tback_ref.at[pl.ds(0, blocks)], text_send.at[way])
            wait_bytes(tback_ref.at[pl.ds(0, partner)], text_recv.at[others])


def exchange(plan, *arrays):
    p = plan
    dma = pltpu.SemaphoreType.DMA
    anywhere = pl.BlockSpec(memory_space=pl.ANY)
    pick = up(p.heads, 8)
    wide = (p.total, p.depth)
    return pl.pallas_call(
        functools.partial(exchange_kernel, p),
        out_shape=(
            jax.ShapeDtypeStruct((p.heads, p.out_rows, p.depth), BF),
            jax.ShapeDtypeStruct((p.heads, p.out_text, p.depth), BF),
            jax.ShapeDtypeStruct((p.images, p.part, p.feature), BF),
        ),
        in_specs=[anywhere] * 13,
        out_specs=(anywhere,) * 3,
        scratch_shapes=[pltpu.VMEM((p.rows, p.feature), BF)] * 4
        + [
            pltpu.VMEM((p.rows, p.model), BF),
            pltpu.VMEM((p.heads, 1, p.rows), F32),
            pltpu.VMEM((p.heads, 1, p.text_rows), F32),
            pltpu.VMEM((p.most, p.out_text, p.depth), BF),
            pltpu.VMEM((p.model, p.feature), BF),
            pltpu.VMEM((5, p.text_rows, p.feature), BF),
            pltpu.VMEM((p.heads, 2, p.rows, p.depth), BF),
            pltpu.VMEM((p.peers, p.stat_rows, p.rows), F32),
            pltpu.VMEM((p.most, 2, *wide), BF),
            pltpu.VMEM((p.peers, p.stat_rows, p.rows), F32),
            pltpu.VMEM((p.stat_rows, p.total - p.tokens), F32),
            pltpu.VMEM((pick, p.rows), F32),
            pltpu.VMEM((pick, p.text_rows), F32),
            pltpu.VMEM(wide, BF),
        ]
        + [pltpu.VMEM(wide, BF)] * 6
        + [
            pltpu.VMEM((p.depth, p.total), F32),
            pltpu.VMEM((p.most, p.peers, p.out_rows, p.depth), BF),
            pltpu.VMEM((2, p.chips, p.share_pad, p.rows), BF),
            pltpu.VMEM((p.chips, p.part, 2 * p.images * p.rows), BF),
            pltpu.VMEM((2 * p.images, p.rows, p.feature), BF),
            pltpu.VMEM((p.chips, p.part, p.feature), BF),
            pltpu.VMEM((p.chips // 2 + 1, p.part, p.feature), BF),
            pltpu.VMEM((p.chips // 2, p.chips // 2, p.part, p.feature), BF),
            dma((9,)), dma((3,)),
            dma((3,)), dma((p.most + 1,)),
            dma((1,)), dma((1,)),
            dma((1,)), dma((1,)),
            dma((3,)), dma((p.chips * p.most + 1,)),
            dma((1,)), dma((2,)),
            dma((1,)), dma((1,)),
            dma((1,)), dma((1,)), dma((1,)),
            dma((1,)), dma((1,)),
        ],
        compiler_params=pltpu.CompilerParams(
            collective_id=0, has_side_effects=True, vmem_limit_bytes=44 << 20
        ),
    )(*(pltpu.with_memory_space_constraint(array, pltpu.HBM) for array in arrays))


def finish_kernel(
    plan, back_ref, tback_ref, parts_ref, dq_out, dk_out, dv_out, tdq_out, tdk_out, tdv_out, wg_out,
    dq_ref, dk_ref, dv_ref, tdq_ref, tdk_ref, tdv_ref, wg_ref, store_sem,
):
    p = plan
    width, rows, half, even = p.width, p.rows, p.text_half, p.text_even
    group = p.heads // p.finish_steps
    stores = []

    def store(source, target):
        copy = pltpu.make_async_copy(source, target, store_sem.at[len(stores)])
        copy.start()
        stores.append(copy)

    whole = [
        pltpu.make_async_copy(source, target, store_sem.at[4 + number])
        for number, (source, target) in enumerate(((tdq_ref, tdq_out), (tdk_ref, tdk_out), (tdv_ref, tdv_out)))
    ]

    for number in range(p.images):
        start = p.part_start(number)
        stop = min(start + p.part, p.share)
        wg_ref[start:stop, :] = parts_ref[number, 0 : stop - start, :].astype(F32)
    store(wg_ref, wg_out)

    def join(ref, pair, at, cols):
        return jnp.concatenate([ref[2 * pair, at, cols], ref[2 * pair + 1, at, cols]], axis=1)

    left, right = slice(0, width), slice(width, p.depth)
    for pair in range(p.heads // 2):
        lanes = slice(pair * p.depth, (pair + 1) * p.depth)
        dq_ref[:, lanes] = join(back_ref, pair, slice(0, rows), left)
        dk_ref[:, lanes] = join(back_ref, pair, slice(0, rows), right)
        dv_ref[0 : rows // 2, lanes] = join(back_ref, pair, slice(rows, p.out_rows), left)
        dv_ref[rows // 2 : rows, lanes] = join(back_ref, pair, slice(rows, p.out_rows), right)
    store(dq_ref, dq_out)
    store(dk_ref, dk_out)
    store(dv_ref, dv_out)
    for step in range(p.finish_steps):
        for pair in range(step * group // 2, (step + 1) * group // 2):
            lanes = slice(pair * p.depth, (pair + 1) * p.depth)
            tdq_ref[:, lanes] = join(tback_ref, pair, slice(0, p.text_rows), left)
            tdk_ref[:, lanes] = join(tback_ref, pair, slice(0, p.text_rows), right)
            tdv_ref[0:half, lanes] = join(tback_ref, pair, slice(even, even + half), left)
            tdv_ref[half : p.text_rows, lanes] = join(tback_ref, pair, slice(even, even + p.text_rows - half), right)
        lanes = slice(step * group * width, (step + 1) * group * width)
        for number, (source, target) in enumerate(((tdq_ref, tdq_out), (tdk_ref, tdk_out), (tdv_ref, tdv_out))):
            pltpu.make_async_copy(source.at[:, lanes], target.at[:, lanes], store_sem.at[4 + number]).start()
    for copy in (*stores, *whole):
        copy.wait()


def finish(plan, back, tback, parts):
    p = plan
    anywhere = pl.BlockSpec(memory_space=pl.ANY)
    token = jax.ShapeDtypeStruct((p.rows, p.feature), BF)
    text = jax.ShapeDtypeStruct((p.text_rows, p.feature), BF)
    outs = (token,) * 3 + (text,) * 3 + (jax.ShapeDtypeStruct((p.share, p.feature), F32),)
    return pl.pallas_call(
        functools.partial(finish_kernel, p),
        out_shape=outs,
        in_specs=[pl.BlockSpec(memory_space=pltpu.VMEM)] * 3,
        out_specs=(anywhere,) * 7,
        scratch_shapes=[pltpu.VMEM(value.shape, value.dtype) for value in outs]
        + [pltpu.SemaphoreType.DMA((7,))],
        compiler_params=pltpu.CompilerParams(vmem_limit_bytes=24 << 20),
    )(back, tback, parts)


def shards(
    image_query,
    image_key,
    image_value,
    image_output,
    output_grad,
    image_logsum,
    text_query,
    text_key,
    text_value,
    text_output,
    text_grad,
    text_logsum,
    out_weight,
):
    plan = Plan(
        lax.axis_size("seq"),
        lax.axis_size("img"),
        image_query.shape[1],
        text_query.shape[1],
        output_grad.shape[2],
        image_query.shape[2],
        image_logsum.shape[2],
    )
    results = exchange(
        plan,
        image_query[0], image_key[0], image_value[0], image_output[0], output_grad[0], image_logsum.transpose(2, 0, 1),
        text_query[0], text_key[0], text_value[0], text_output[0], text_grad[0], text_logsum.transpose(2, 0, 1),
        out_weight,
    )
    *grads, weight_grad = finish(plan, *results)
    return (*(grad[None] for grad in grads), weight_grad)


def solution(mesh):
    token = P("img", "seq", None)
    text = P("img", None, None)
    return jax.shard_map(
        shards,
        mesh=mesh,
        in_specs=(token,) * 6 + (text,) * 6 + (P(),),
        out_specs=(token,) * 3 + (text,) * 3 + (P("seq", None),),
        check_vma=False,
    )
```

```python
import functools

import jax
import jax.numpy as jnp
from jax import lax
from jax.experimental import pallas as pl
from jax.experimental.pallas import tpu as pltpu
from jax.sharding import PartitionSpec as P

LANES = 128
SUB = 16
MESH = pl.DeviceIdType.MESH
NN = (((1,), (0,)), ((), ()))
NT = (((1,), (1,)), ((), ()))
TN = (((0,), (0,)), ((), ()))
BF = jnp.bfloat16
F32 = jnp.float32


def up(value, step):
    return -(-value // step) * step


class Plan:
    def __init__(self, peers, images, rows, text_rows, model, feature, heads):
        self.peers, self.images, self.rows = peers, images, rows
        self.text_rows, self.model, self.feature, self.heads = text_rows, model, feature, heads
        self.chips = peers // 2
        self.width = feature // heads
        self.depth = 2 * self.width
        self.most = -(-heads // peers)
        self.stat_rows = up(2 * self.most, 8)
        self.tokens = peers * rows
        self.total = self.tokens + up(text_rows, LANES)
        self.key_block = self.total // 8
        self.text_even = up(text_rows, SUB)
        self.text_half = up(self.text_even // 2, SUB)
        self.out_rows = rows + rows // 2
        self.out_text = self.text_even + self.text_half
        self.share = model // peers
        self.finish_steps = next(n for n in (5, 4, 3, 2, 1) if heads % (2 * n) == 0)
        self.share_pad = up(self.share, SUB)
        self.part = up(-(-self.share_pad // images), SUB)

    def first(self, device):
        return device * self.heads // self.peers

    def part_start(self, image):
        if isinstance(image, int):
            return min(image * self.part, self.share_pad - self.part)
        return pl.multiple_of(jnp.minimum(image * self.part, self.share_pad - self.part), SUB)


def exchange_kernel(
    plan,
    q_in, k_in, v_in, o_in, og_in_ref, ls_in,
    tq_ref, tk_ref, tv_ref, to_ref, tg_ref, tls_in, w_ref,
    back_ref, tback_ref, parts_ref,
    q_ref, k_ref, v_ref, o_ref, og_ref, ls_ref, tls_ref, text_s, w_s, txt_s, x_out, st_out, x_in, st_in, st_text, dots_s, tdots_s, stat_s,
    q_s, k_s, v_s, g_s, dk_s, dv_s, dq_s, result_s, ogt_s, og_in, io_in, sums_out, sums_in, gate_in,
    local_sem, own_sem, x_send, x_recv, st_send, st_recv, back_send, back_recv,
    text_send, text_recv, io_send, io_recv, og_send, og_recv, sums_send, sums_recv, gate_recv,
    parts_send, parts_recv,
):
    p = plan
    peers, images, rows, width, depth, chips = p.peers, p.images, p.rows, p.width, p.depth, p.chips
    scaling = width ** (-0.5)
    me = lax.axis_index("seq")
    image = lax.axis_index("img")
    chip, core = me // 2, me % 2
    first = p.first(me)
    count = p.first(me + 1) - first
    slot = image * 2 + core
    my_rows = pl.ds(pl.multiple_of(me * rows, rows), rows)

    def remote(source, target, send, recv, device):
        return pltpu.make_async_remote_copy(
            src_ref=source, dst_ref=target, send_sem=send, recv_sem=recv,
            device_id=device, device_id_type=MESH,
        )

    barrier = pltpu.get_barrier_semaphore()

    @pl.loop(1, peers)
    def _(step):
        pl.semaphore_signal(barrier, inc=1, device_id=(image, (me + step) % peers), device_id_type=MESH)

    @pl.loop(1, images)
    def _(step):
        for side in range(2):
            pl.semaphore_signal(
                barrier, inc=1, device_id=((image + step) % images, chip * 2 + side), device_id_type=MESH
            )

    pairs = {
        "q": (q_in, q_ref), "k": (k_in, k_ref), "o": (o_in, o_ref), "og": (og_in_ref, og_ref), "w": (w_ref, w_s),
        "v": (v_in, v_ref), "ls": (ls_in, ls_ref), "tls": (tls_in, tls_ref),
    }
    loads = {}
    for number, (name, (source, target)) in enumerate(pairs.items()):
        loads[name] = pltpu.make_async_copy(source, target, local_sem.at[number])
        loads[name].start()
    for number, source in enumerate((tq_ref, tk_ref, tv_ref, tg_ref, to_ref)):
        pltpu.make_async_copy(source, txt_s.at[number], local_sem.at[len(pairs)]).start()

    def wait_bytes(ref, sem):
        pltpu.make_async_copy(ref, ref, sem).wait()

    loads["q"].wait()
    loads["k"].wait()

    for head in range(p.heads):
        cols = slice(head * width, (head + 1) * width)
        x_out[head, 0] = jnp.concatenate([q_ref[:, cols] * jnp.asarray(scaling, BF), k_ref[:, cols]], axis=1)

    pl.semaphore_wait(barrier, peers - 1 + 2 * (images - 1))

    def targets(j, action):
        @pl.loop(0, peers)
        def _(step):
            device = (me + peers // 2 + step) % peers
            head = p.first(device) + j

            @pl.when((device != me) & (head < p.first(device + 1)))
            def _():
                action(device, head)

    def copy_x(j, part):
        if j == 0:
            return lambda device, head: remote(
                x_out.at[head, part], x_in.at[j, part, my_rows], x_send.at[part], x_recv.at[part], (image, device)
            )
        return lambda device, head: remote(
            x_out.at[head], x_in.at[j, :, my_rows], x_send.at[2], x_recv.at[1 + j], (image, device)
        )

    def copy_st(device):
        return remote(st_out.at[device], st_in.at[me], st_send.at[0], st_recv.at[0], (image, device))

    targets(0, lambda device, head: copy_x(0, 0)(device, head).start())

    loads["o"].wait()
    loads["og"].wait()

    def copy_io(step):
        return remote(
            o_ref, io_in.at[slot], io_send.at[0], io_recv.at[0], ((image + step) % images, me)
        )

    def share_io(step):
        source = ((image + step) % images) * 2 + core
        return remote(
            io_in.at[source], io_in.at[source], io_send.at[0], io_recv.at[1],
            (image, chip * 2 + 1 - core),
        )

    copy_own = remote(
        o_ref, io_in.at[slot], io_send.at[0], io_recv.at[1], (image, chip * 2 + 1 - core)
    )

    @pl.loop(1, images)
    def _(step):
        copy_io(step).start()

    copy_own.start()

    for number in range(-(-p.model // LANES)):
        lanes = slice(number * LANES, (number + 1) * LANES)
        dq_s[:, 0:rows] = jnp.zeros((LANES, rows), F32) + og_ref[:, lanes].astype(F32).T
        turned = dq_s[:, 0:rows]
        for device in range(peers):
            low = max(number * LANES, device * p.share)
            high = min((number + 1) * LANES, (device + 1) * p.share)
            if low < high:
                ogt_s[device % 2, device // 2, low - device * p.share : high - device * p.share, :] = turned[
                    low - number * LANES : high - number * LANES
                ].astype(BF)

    def copy_og(step, side):
        other = (image + step) % images
        return remote(
            ogt_s.at[side, :, pl.ds(p.part_start(other), p.part)],
            og_in.at[:, :, pl.ds(pl.multiple_of(slot * rows, rows), rows)],
            og_send.at[0],
            og_recv.at[0],
            (other, chip * 2 + side),
        )

    @pl.loop(1, images)
    def _(step):
        for side in range(2):
            copy_og(step, side).start()

    for side in range(2):
        @pl.when(core != side)
        def _():
            copy_og(0, side).start()

    og_in[:, :, pl.ds(pl.multiple_of(slot * rows, rows), rows)] = ogt_s[
        core, :, pl.ds(p.part_start(image), p.part)
    ]
    io_in[slot] = o_ref[...]

    loads["w"].wait()

    @pl.loop(0, p.feature // 256)
    def _(step):
        lanes = pl.ds(pl.multiple_of(step * 256, 256), 256)
        g_cols = jnp.dot(og_ref[...], w_s[:, lanes], preferred_element_type=F32).astype(BF)
        per = 256 // width
        for number in range(per):
            head = step * per + number
            x_out[head, 1, :, 0:width] = g_cols[:, number * width : (number + 1) * width]

    pick_rows = up(p.heads, 8)
    tag = lax.broadcasted_iota(jnp.int32, (pick_rows, p.feature), 0)
    lane_at = lax.broadcasted_iota(jnp.int32, (pick_rows, p.feature), 1)
    picker = jnp.where((lane_at >= tag * width) & (lane_at < (tag + 1) * width), 1.0, 0.0).astype(F32)

    def row_dots(grads, outputs):
        product = grads.astype(F32) * outputs.astype(F32)
        return lax.dot_general(
            picker, product, NT, precision=lax.Precision.HIGHEST, preferred_element_type=F32
        )

    gathered = jnp.concatenate([x_out[head, 1, :, 0:width] for head in range(p.heads)], axis=1)
    dots_s[...] = row_dots(gathered, o_ref[...])
    loads["v"].wait()
    loads["ls"].wait()
    for head in range(p.heads):
        x_out[head, 1, :, width:depth] = v_ref[:, head * width : (head + 1) * width]
    st_out[...] = jnp.zeros_like(st_out)
    for device in range(peers):
        for j in range(p.first(device + 1) - p.first(device)):
            head = p.first(device) + j
            st_out[device, 2 * j : 2 * j + 1, :] = -ls_ref[head]
            st_out[device, 2 * j + 1 : 2 * j + 2, :] = -dots_s[head : head + 1, :]

    @pl.loop(0, peers)
    def _(step):
        device = (me + peers // 2 + step) % peers

        @pl.when(device != me)
        def _():
            copy_st(device).start()

    targets(0, lambda device, head: copy_x(0, 1)(device, head).start())
    for j in range(1, p.most):
        targets(j, lambda device, head: copy_x(j, 0)(device, head).start())

    loads["tls"].wait()
    wait_bytes(txt_s, local_sem.at[len(pairs)])
    tdots_s[...] = row_dots(txt_s[3], txt_s[4])
    st_text[...] = jnp.zeros_like(st_text)
    text_at = slice(p.tokens, p.tokens + p.text_rows)
    pad_at = slice(p.tokens + p.text_rows // SUB * SUB, p.total)

    @pl.loop(0, count)
    def _(j):
        head = first + j
        tile = pl.ds(pl.multiple_of(head // 2 * depth, depth), depth)
        odd = head % 2 == 1

        def text_cols(number):
            value = txt_s[number, :, tile]
            return jnp.where(odd, value[:, width:], value[:, :width])

        x_in[j, 0, my_rows] = x_out[head, 0]
        x_in[j, 1, my_rows] = x_out[head, 1]
        x_in[j, 0, pad_at] = jnp.zeros((p.total - pad_at.start, depth), BF)
        x_in[j, 1, pad_at] = jnp.zeros((p.total - pad_at.start, depth), BF)
        x_in[j, 0, text_at] = jnp.concatenate([text_cols(0) * jnp.asarray(scaling, BF), text_cols(1)], axis=1)
        x_in[j, 1, text_at] = jnp.concatenate([text_cols(3), text_cols(2)], axis=1)
        st_text[pl.ds(2 * j, 1), 0 : p.text_rows] = -tls_ref[head]
        st_text[pl.ds(2 * j + 1, 1), 0 : p.text_rows] = -tdots_s[pl.ds(head, 1), :]

    def stats_tile(value):
        terms = []
        for _ in range(3):
            term = value.astype(BF).astype(F32)
            terms.append(term)
            value = value - term
        used = width + 3 * p.stat_rows
        return jnp.concatenate(
            [jnp.zeros((width, LANES), F32), *terms, jnp.zeros((depth - used, LANES), F32)], axis=0
        ).T.astype(BF)

    for number in range((p.total - p.tokens) // LANES):
        stat_s[p.tokens + number * LANES : p.tokens + (number + 1) * LANES, :] = stats_tile(
            st_text[:, number * LANES : (number + 1) * LANES]
        )

    st_in[me] = st_out[me]

    wait_bytes(st_in.at[pl.ds(0, peers - 1)], st_recv.at[0])

    @pl.loop(0, peers)
    def _(source):
        stat_s[pl.ds(pl.multiple_of(source * rows, rows), rows), :] = stats_tile(st_in[source])

    lane = lax.broadcasted_iota(jnp.int32, (p.total, depth), 1)

    def ones(start):
        inside = (lane == width + start)
        for number in range(1, 3):
            inside = inside | (lane == width + start + number * p.stat_rows)
        return jnp.where(inside, 1.0, 0.0).astype(BF)[:, width:]

    far = pl.ds(0, (peers - 1) * rows)

    others = chips * p.most

    def text_slot(head, owner):
        return owner // 2 * p.most + head - p.first(owner)

    def send_text(source, head, owner, upward, downward):
        def send(way, recv, device):
            remote(source, tback_ref.at[head], text_send.at[way], text_recv.at[recv], (image, device)).start()

        @pl.when(upward & (chip + 1 < chips))
        def _():
            send(0, text_slot(head, owner), me + 2)

        @pl.when(downward & (chip > 0))
        def _():
            send(1, text_slot(head, owner), me - 2)

        send(2, others, chip * 2 + 1 - core)

    def own_back(j):
        return pltpu.make_async_copy(result_s.at[j, me], back_ref.at[first + j], own_sem.at[0])

    def ordered(head, value):
        return jnp.where(head % 2 == 1, jnp.concatenate([value[:, width:], value[:, :width]], axis=1), value)

    def send_back(j):
        own_back(j).start()

        @pl.loop(0, peers)
        def _(step):
            block = (me + peers // 2 + step) % peers

            @pl.when(block != me)
            def _():
                remote(
                    result_s.at[j, block], back_ref.at[first + j], back_send.at[0], back_recv.at[0],
                    (image, block),
                ).start()

    def own_text(j):
        return pltpu.make_async_copy(text_s.at[j], tback_ref.at[first + j], own_sem.at[1])

    half_chips = chips // 2
    side, seat = chip // half_chips, chip % half_chips
    gate = half_chips - 1 + side
    near, beyond = side * half_chips, (1 - side) * half_chips
    edge = chip != gate

    def send_sum(number, target, recv, device):
        remote(
            sums_out.at[number], target, sums_send.at[0], recv, (image, device * 2 + core)
        ).start()

    def send_terms():
        for number in range(half_chips):
            @pl.when(edge)
            def _():
                send_sum(beyond + number, gate_in.at[seat, number], gate_recv.at[0], gate)

        for number in range(half_chips):
            @pl.when(number != seat)
            def _():
                send_sum(near + number, sums_in.at[seat], sums_recv.at[0], near + number)

    def pass_sums():
        @pl.when(chip == gate)
        def _():
            if half_chips > 1:
                wait_bytes(gate_in.at[pl.ds(0, half_chips - 1)], gate_recv.at[0])
            for number in range(half_chips):
                @pl.loop(1, half_chips)
                def _(step):
                    source = (seat + step) % half_chips

                    @pl.loop(0, p.feature // 256)
                    def _(step):
                        lanes = pl.ds(pl.multiple_of(step * 256, 256), 256)
                        total = sums_out[beyond + number, :, lanes].astype(F32)
                        total += gate_in[source, number, :, lanes].astype(F32)
                        sums_out[beyond + number, :, lanes] = total.astype(BF)

                send_sum(beyond + number, sums_in.at[half_chips], sums_recv.at[0], beyond + number)

    def pass_text(hop, low, high, inward=(True, False)):
        for upward in (True, False):
            source = chip - hop if upward else chip + hop
            inner = side == (0 if upward else 1)
            wanted = {(True,): inner, (False,): ~inner}.get(inward, True)

            @pl.when((source >= 0) & (source < chips) & wanted)
            def _():
                owner = source * 2 + core
                start, stop = p.first(owner), p.first(owner + 1)

                @pl.loop(start + low, jnp.minimum(stop, start + high))
                def _(head):
                    wait_bytes(tback_ref.at[head], text_recv.at[text_slot(head, owner)])
                    send_text(tback_ref.at[head], head, owner, upward, not upward)

    @pl.loop(0, count)
    def _(j):
        head = first + j
        @pl.when(j == 0)
        def _():
            for part in range(2):
                wait_bytes(x_in.at[0, part, far], x_recv.at[part])

        @pl.when(j > 0)
        def _():
            wait_bytes(x_in.at[j, :, far], x_recv.at[1 + j])

        both = x_in[j, 0]
        q_s[...] = jnp.where(lane < width, both, stat_s[...])
        k_s[...] = jnp.concatenate([both[:, width:], ones(2 * j)], axis=1)
        both = x_in[j, 1]
        g_s[...] = jnp.where(lane < width, both, stat_s[...])
        v_s[...] = jnp.concatenate([both[:, width:], ones(2 * j + 1)], axis=1)
        dq_s[...] = jnp.zeros_like(dq_s)

        @pl.loop(0, p.total // p.key_block)
        def _(step):
            at = pl.ds(pl.multiple_of(step * p.key_block, p.key_block), p.key_block)
            keys = k_s[at, :]
            scores = lax.dot_general(keys, q_s[...], NT, preferred_element_type=F32)
            weights = jnp.exp(scores)
            grads = lax.dot_general(v_s[at, :], g_s[...], NT, preferred_element_type=F32)
            low = (weights * grads).astype(BF)
            dv_s[at, :] = jnp.dot(weights.astype(BF), g_s[...], preferred_element_type=F32).astype(BF)
            dk_s[at, :] = jnp.dot(low, q_s[...], preferred_element_type=F32).astype(BF)
            dq_s[...] += lax.dot_general(keys, low, TN, preferred_element_type=F32)

        dq = (dq_s[:, p.tokens : p.total].T * scaling).astype(BF)
        even, half = p.text_even, p.text_half
        top = jnp.concatenate([dq[:even, :width], dk_s[p.tokens : p.tokens + even, :width]], axis=1)
        bottom = jnp.concatenate(
            [dv_s[p.tokens : p.tokens + half, :width], dv_s[p.tokens + half : p.tokens + 2 * half, :width]],
            axis=1,
        )
        text_s[j, 0:even] = ordered(head, top)
        text_s[j, even : even + half] = ordered(head, bottom)
        own_text(j).start()
        send_text(text_s.at[j], head, me, True, True)

        @pl.when(j == 0)
        def _():
            if images > 1:
                wait_bytes(io_in.at[pl.ds(0, images - 1)], io_recv.at[0])

            @pl.loop(1, images)
            def _(step):
                share_io(step).start()

        @pl.when(j == 0)
        def _():
            wait_bytes(io_in.at[pl.ds(0, images)], io_recv.at[1])
            wait_bytes(og_in.at[:, :, pl.ds(0, (2 * images - 1) * rows)], og_recv.at[0])

            @pl.loop(0, p.feature // 256)
            def _(step):
                lanes = pl.ds(pl.multiple_of(step * 256, 256), 256)
                for number in range(chips):
                    total = jnp.zeros((p.part, 256), F32)
                    for source in range(2 * images):
                        total += jnp.dot(
                            og_in[number, :, source * rows : (source + 1) * rows],
                            io_in[source, :, lanes],
                            preferred_element_type=F32,
                        )
                    sums_out[number, :, lanes] = total.astype(BF)

            send_terms()

        @pl.loop(0, peers)
        def _(block):
            base = pl.multiple_of(block * rows, rows)
            dq = (dq_s[:, pl.ds(base, rows)].T * scaling).astype(BF)
            top = jnp.concatenate([dq[:, :width], dk_s[pl.ds(base, rows), :width]], axis=1)
            dv = dv_s[pl.ds(base, rows), :width]
            bottom = jnp.concatenate([dv[: rows // 2], dv[rows // 2 :]], axis=1)
            result_s[j, block, 0:rows] = ordered(head, top)
            result_s[j, block, rows : p.out_rows] = ordered(head, bottom)

        @pl.when(j == 0)
        def _():
            pass_text(1, 0, 1)

        @pl.when(j == jnp.minimum(1, count - 1))
        def _():
            pass_sums()

        @pl.when(j == jnp.where(edge, jnp.minimum(1, count - 1), 0))
        def _():
            send_back(0)


    pass_text(1, 1, p.most, (True,))

    @pl.loop(1, count)
    def _(j):
        send_back(j)

    pass_text(1, 1, 2, (False,))
    if chips > 2:
        pass_text(2, 0, 1)
    pass_text(1, 2, p.most, (False,))

    wait_bytes(sums_in.at[pl.ds(0, half_chips)], sums_recv.at[0])

    @pl.loop(0, half_chips + 1)
    def _(source):
        @pl.when(source != seat)
        def _():
            @pl.loop(0, p.feature // 256)
            def _(step):
                lanes = pl.ds(pl.multiple_of(step * 256, 256), 256)
                total = sums_out[chip, :, lanes].astype(F32) + sums_in[source, :, lanes].astype(F32)
                sums_out[chip, :, lanes] = total.astype(BF)

    own_parts = pltpu.make_async_copy(sums_out.at[chip], parts_ref.at[image], own_sem.at[2])
    own_parts.start()

    def copy_parts(step):
        return remote(
            sums_out.at[chip], parts_ref.at[image], parts_send.at[0], parts_recv.at[0],
            ((image + step) % images, me),
        )

    @pl.loop(1, images)
    def _(step):
        copy_parts(step).start()

    if chips > 2:
        pass_text(2, 1, p.most)
    for hop in range(3, chips):
        pass_text(hop, 0, p.most)

    own_parts.wait()
    if images > 1:
        wait_bytes(parts_ref.at[pl.ds(0, images - 1)], parts_recv.at[0])
        wait_bytes(parts_ref.at[pl.ds(0, images - 1)], parts_send.at[0])
    wait_bytes(io_in.at[pl.ds(0, 2 * images - 1)], io_send.at[0])
    wait_bytes(og_in.at[:, :, pl.ds(0, (2 * images - 1) * rows)], og_send.at[0])
    wait_bytes(st_in.at[pl.ds(0, peers - 1)], st_send.at[0])
    if chips > 1:
        wait_bytes(sums_out.at[pl.ds(0, chips - 1)], sums_send.at[0])

    def heads_of(number, side):
        return p.first(number * 2 + side + 1) - p.first(number * 2 + side)

    for device in range(peers):
        here, at = device // 2, device % 2
        mine = heads_of(here, at)
        same = [heads_of(number, at) for number in range(chips)]
        upward = sum(same[: here + 1]) if here + 1 < chips else 0
        downward = sum(same[here:]) if here > 0 else 0
        partner = p.heads - sum(same)

        @pl.when(me == device)
        def _():
            wait_bytes(back_ref.at[pl.ds(0, mine)], own_sem.at[0])
            wait_bytes(tback_ref.at[pl.ds(0, mine)], own_sem.at[1])
            for part in range(2):
                wait_bytes(x_out.at[pl.ds(0, peers - 1), part], x_send.at[part])
            if p.heads - peers > mine - 1:
                wait_bytes(x_out.at[pl.ds(0, p.heads - peers - mine + 1)], x_send.at[2])
            wait_bytes(result_s.at[pl.ds(0, mine), pl.ds(0, peers - 1)], back_send.at[0])
            wait_bytes(back_ref.at[pl.ds(0, p.heads - mine)], back_recv.at[0])
            for way, blocks in enumerate((upward, downward, sum(same))):
                if blocks:
                    wait_bytes(tback_ref.at[pl.ds(0, blocks)], text_send.at[way])
            wait_bytes(tback_ref.at[pl.ds(0, partner)], text_recv.at[others])


def exchange(plan, *arrays):
    p = plan
    dma = pltpu.SemaphoreType.DMA
    anywhere = pl.BlockSpec(memory_space=pl.ANY)
    pick = up(p.heads, 8)
    wide = (p.total, p.depth)
    return pl.pallas_call(
        functools.partial(exchange_kernel, p),
        out_shape=(
            jax.ShapeDtypeStruct((p.heads, p.out_rows, p.depth), BF),
            jax.ShapeDtypeStruct((p.heads, p.out_text, p.depth), BF),
            jax.ShapeDtypeStruct((p.images, p.part, p.feature), BF),
        ),
        in_specs=[anywhere] * 13,
        out_specs=(anywhere,) * 3,
        scratch_shapes=[pltpu.VMEM((p.rows, p.feature), BF)] * 4
        + [
            pltpu.VMEM((p.rows, p.model), BF),
            pltpu.VMEM((p.heads, 1, p.rows), F32),
            pltpu.VMEM((p.heads, 1, p.text_rows), F32),
            pltpu.VMEM((p.most, p.out_text, p.depth), BF),
            pltpu.VMEM((p.model, p.feature), BF),
            pltpu.VMEM((5, p.text_rows, p.feature), BF),
            pltpu.VMEM((p.heads, 2, p.rows, p.depth), BF),
            pltpu.VMEM((p.peers, p.stat_rows, p.rows), F32),
            pltpu.VMEM((p.most, 2, *wide), BF),
            pltpu.VMEM((p.peers, p.stat_rows, p.rows), F32),
            pltpu.VMEM((p.stat_rows, p.total - p.tokens), F32),
            pltpu.VMEM((pick, p.rows), F32),
            pltpu.VMEM((pick, p.text_rows), F32),
            pltpu.VMEM(wide, BF),
        ]
        + [pltpu.VMEM(wide, BF)] * 6
        + [
            pltpu.VMEM((p.depth, p.total), F32),
            pltpu.VMEM((p.most, p.peers, p.out_rows, p.depth), BF),
            pltpu.VMEM((2, p.chips, p.share_pad, p.rows), BF),
            pltpu.VMEM((p.chips, p.part, 2 * p.images * p.rows), BF),
            pltpu.VMEM((2 * p.images, p.rows, p.feature), BF),
            pltpu.VMEM((p.chips, p.part, p.feature), BF),
            pltpu.VMEM((p.chips // 2 + 1, p.part, p.feature), BF),
            pltpu.VMEM((p.chips // 2, p.chips // 2, p.part, p.feature), BF),
            dma((9,)), dma((3,)),
            dma((3,)), dma((p.most + 1,)),
            dma((1,)), dma((1,)),
            dma((1,)), dma((1,)),
            dma((3,)), dma((p.chips * p.most + 1,)),
            dma((1,)), dma((2,)),
            dma((1,)), dma((1,)),
            dma((1,)), dma((1,)), dma((1,)),
            dma((1,)), dma((1,)),
        ],
        compiler_params=pltpu.CompilerParams(
            collective_id=0, has_side_effects=True, vmem_limit_bytes=44 << 20
        ),
    )(*(pltpu.with_memory_space_constraint(array, pltpu.HBM) for array in arrays))


def finish_kernel(
    plan, back_ref, tback_ref, parts_ref, dq_out, dk_out, dv_out, tdq_out, tdk_out, tdv_out, wg_out,
    dq_ref, dk_ref, dv_ref, tdq_ref, tdk_ref, tdv_ref, wg_ref, store_sem,
):
    p = plan
    width, rows, half, even = p.width, p.rows, p.text_half, p.text_even
    group = p.heads // p.finish_steps
    stores = []

    def store(source, target):
        copy = pltpu.make_async_copy(source, target, store_sem.at[len(stores)])
        copy.start()
        stores.append(copy)

    whole = [
        pltpu.make_async_copy(source, target, store_sem.at[4 + number])
        for number, (source, target) in enumerate(((tdq_ref, tdq_out), (tdk_ref, tdk_out), (tdv_ref, tdv_out)))
    ]

    for number in range(p.images):
        start = p.part_start(number)
        stop = min(start + p.part, p.share)
        wg_ref[start:stop, :] = parts_ref[number, 0 : stop - start, :].astype(F32)
    store(wg_ref, wg_out)

    def join(ref, pair, at, left):
        even_head, odd_head = ref[2 * pair, at, :], ref[2 * pair + 1, at, :]
        lower = lax.broadcasted_iota(jnp.int32, even_head.shape, 1) < width
        if left:
            return jnp.where(lower, even_head, odd_head)
        mixed = jnp.where(lower, odd_head, even_head)
        return jnp.concatenate([mixed[:, width:], mixed[:, :width]], axis=1)

    left, right = True, False
    for pair in range(p.heads // 2):
        lanes = slice(pair * p.depth, (pair + 1) * p.depth)
        dq_ref[:, lanes] = join(back_ref, pair, slice(0, rows), left)
        dk_ref[:, lanes] = join(back_ref, pair, slice(0, rows), right)
        dv_ref[0 : rows // 2, lanes] = join(back_ref, pair, slice(rows, p.out_rows), left)
        dv_ref[rows // 2 : rows, lanes] = join(back_ref, pair, slice(rows, p.out_rows), right)
    store(dq_ref, dq_out)
    store(dk_ref, dk_out)
    store(dv_ref, dv_out)
    for step in range(p.finish_steps):
        for pair in range(step * group // 2, (step + 1) * group // 2):
            lanes = slice(pair * p.depth, (pair + 1) * p.depth)
            tdq_ref[:, lanes] = join(tback_ref, pair, slice(0, p.text_rows), left)
            tdk_ref[:, lanes] = join(tback_ref, pair, slice(0, p.text_rows), right)
            tdv_ref[0:half, lanes] = join(tback_ref, pair, slice(even, even + half), left)
            tdv_ref[half : p.text_rows, lanes] = join(tback_ref, pair, slice(even, even + p.text_rows - half), right)
        lanes = slice(step * group * width, (step + 1) * group * width)
        for number, (source, target) in enumerate(((tdq_ref, tdq_out), (tdk_ref, tdk_out), (tdv_ref, tdv_out))):
            pltpu.make_async_copy(source.at[:, lanes], target.at[:, lanes], store_sem.at[4 + number]).start()
    for copy in (*stores, *whole):
        copy.wait()


def finish(plan, back, tback, parts):
    p = plan
    anywhere = pl.BlockSpec(memory_space=pl.ANY)
    token = jax.ShapeDtypeStruct((p.rows, p.feature), BF)
    text = jax.ShapeDtypeStruct((p.text_rows, p.feature), BF)
    outs = (token,) * 3 + (text,) * 3 + (jax.ShapeDtypeStruct((p.share, p.feature), F32),)
    return pl.pallas_call(
        functools.partial(finish_kernel, p),
        out_shape=outs,
        in_specs=[pl.BlockSpec(memory_space=pltpu.VMEM)] * 3,
        out_specs=(anywhere,) * 7,
        scratch_shapes=[pltpu.VMEM(value.shape, value.dtype) for value in outs]
        + [pltpu.SemaphoreType.DMA((7,))],
        compiler_params=pltpu.CompilerParams(vmem_limit_bytes=24 << 20),
    )(back, tback, parts)


def shards(
    image_query,
    image_key,
    image_value,
    image_output,
    output_grad,
    image_logsum,
    text_query,
    text_key,
    text_value,
    text_output,
    text_grad,
    text_logsum,
    out_weight,
):
    plan = Plan(
        lax.axis_size("seq"),
        lax.axis_size("img"),
        image_query.shape[1],
        text_query.shape[1],
        output_grad.shape[2],
        image_query.shape[2],
        image_logsum.shape[2],
    )
    results = exchange(
        plan,
        image_query[0], image_key[0], image_value[0], image_output[0], output_grad[0], image_logsum.transpose(2, 0, 1),
        text_query[0], text_key[0], text_value[0], text_output[0], text_grad[0], text_logsum.transpose(2, 0, 1),
        out_weight,
    )
    *grads, weight_grad = finish(plan, *results)
    return (*(grad[None] for grad in grads), weight_grad)


def solution(mesh):
    token = P("img", "seq", None)
    text = P("img", None, None)
    return jax.shard_map(
        shards,
        mesh=mesh,
        in_specs=(token,) * 6 + (text,) * 6 + (P(),),
        out_specs=(token,) * 3 + (text,) * 3 + (P("seq", None),),
        check_vma=False,
    )
```

```python
import functools

import jax
import jax.numpy as jnp
from jax import lax
from jax.experimental import pallas as pl
from jax.experimental.pallas import tpu as pltpu
from jax.sharding import PartitionSpec as P

LANES = 128
SUB = 16
MESH = pl.DeviceIdType.MESH
NN = (((1,), (0,)), ((), ()))
NT = (((1,), (1,)), ((), ()))
TN = (((0,), (0,)), ((), ()))
BF = jnp.bfloat16
F32 = jnp.float32


def up(value, step):
    return -(-value // step) * step


class Plan:
    def __init__(self, peers, images, rows, text_rows, model, feature, heads):
        self.peers, self.images, self.rows = peers, images, rows
        self.text_rows, self.model, self.feature, self.heads = text_rows, model, feature, heads
        self.chips = peers // 2
        self.width = feature // heads
        self.depth = 2 * self.width
        self.most = -(-heads // peers)
        self.stat_rows = up(2 * self.most, 8)
        self.tokens = peers * rows
        self.total = self.tokens + up(text_rows, LANES)
        self.key_block = self.total // 8
        self.text_even = up(text_rows, SUB)
        self.text_half = up(self.text_even // 2, 8)
        self.out_rows = rows + rows // 2
        self.out_text = self.text_even + self.text_half
        self.share = model // peers
        self.finish_steps = next(n for n in (5, 4, 3, 2, 1) if heads % (2 * n) == 0)
        self.share_pad = up(self.share, SUB)
        self.part = up(-(-self.share_pad // images), SUB)

    def first(self, device):
        return device * self.heads // self.peers

    def part_start(self, image):
        if isinstance(image, int):
            return min(image * self.part, self.share_pad - self.part)
        return pl.multiple_of(jnp.minimum(image * self.part, self.share_pad - self.part), SUB)


def exchange_kernel(
    plan,
    q_in, k_in, v_in, o_in, og_in_ref, ls_in,
    tq_ref, tk_ref, tv_ref, to_ref, tg_ref, tls_in, w_ref,
    back_ref, tback_ref, parts_ref,
    q_ref, k_ref, v_ref, o_ref, og_ref, ls_ref, tls_ref, text_s, w_s, txt_s, x_out, st_out, x_in, st_in, st_text, dots_s, tdots_s, stat_s,
    q_s, k_s, v_s, g_s, dk_s, dv_s, dq_s, result_s, ogt_s, og_in, io_in, sums_out, sums_in, gate_in,
    local_sem, own_sem, x_send, x_recv, st_send, st_recv, back_send, back_recv,
    text_send, text_recv, io_send, io_recv, og_send, og_recv, sums_send, sums_recv, gate_recv,
    parts_send, parts_recv,
):
    p = plan
    peers, images, rows, width, depth, chips = p.peers, p.images, p.rows, p.width, p.depth, p.chips
    scaling = width ** (-0.5)
    me = lax.axis_index("seq")
    image = lax.axis_index("img")
    chip, core = me // 2, me % 2
    first = p.first(me)
    count = p.first(me + 1) - first
    slot = image * 2 + core
    my_rows = pl.ds(pl.multiple_of(me * rows, rows), rows)

    def remote(source, target, send, recv, device):
        return pltpu.make_async_remote_copy(
            src_ref=source, dst_ref=target, send_sem=send, recv_sem=recv,
            device_id=device, device_id_type=MESH,
        )

    barrier = pltpu.get_barrier_semaphore()

    @pl.loop(1, peers)
    def _(step):
        pl.semaphore_signal(barrier, inc=1, device_id=(image, (me + step) % peers), device_id_type=MESH)

    @pl.loop(1, images)
    def _(step):
        for side in range(2):
            pl.semaphore_signal(
                barrier, inc=1, device_id=((image + step) % images, chip * 2 + side), device_id_type=MESH
            )

    pairs = {
        "q": (q_in, q_ref), "k": (k_in, k_ref), "o": (o_in, o_ref), "og": (og_in_ref, og_ref), "w": (w_ref, w_s),
        "v": (v_in, v_ref), "ls": (ls_in, ls_ref), "tls": (tls_in, tls_ref),
    }
    loads = {}
    for number, (name, (source, target)) in enumerate(pairs.items()):
        loads[name] = pltpu.make_async_copy(source, target, local_sem.at[number])
        loads[name].start()
    for number, source in enumerate((tq_ref, tk_ref, tv_ref, tg_ref, to_ref)):
        pltpu.make_async_copy(source, txt_s.at[number], local_sem.at[len(pairs)]).start()

    def wait_bytes(ref, sem):
        pltpu.make_async_copy(ref, ref, sem).wait()

    loads["q"].wait()
    loads["k"].wait()

    for head in range(p.heads):
        cols = slice(head * width, (head + 1) * width)
        x_out[head, 0] = jnp.concatenate([q_ref[:, cols] * jnp.asarray(scaling, BF), k_ref[:, cols]], axis=1)

    pl.semaphore_wait(barrier, peers - 1 + 2 * (images - 1))

    def targets(j, action):
        @pl.loop(0, peers)
        def _(step):
            device = (me + peers // 2 + step) % peers
            head = p.first(device) + j

            @pl.when((device != me) & (head < p.first(device + 1)))
            def _():
                action(device, head)

    def copy_x(j, part):
        if j == 0:
            return lambda device, head: remote(
                x_out.at[head, part], x_in.at[j, part, my_rows], x_send.at[part], x_recv.at[part], (image, device)
            )
        return lambda device, head: remote(
            x_out.at[head], x_in.at[j, :, my_rows], x_send.at[2], x_recv.at[1 + j], (image, device)
        )

    def copy_st(device):
        return remote(st_out.at[device], st_in.at[me], st_send.at[0], st_recv.at[0], (image, device))

    targets(0, lambda device, head: copy_x(0, 0)(device, head).start())

    loads["o"].wait()
    loads["og"].wait()

    def copy_io(step):
        return remote(
            o_ref, io_in.at[slot], io_send.at[0], io_recv.at[0], ((image + step) % images, me)
        )

    def share_io(step):
        source = ((image + step) % images) * 2 + core
        return remote(
            io_in.at[source], io_in.at[source], io_send.at[0], io_recv.at[1],
            (image, chip * 2 + 1 - core),
        )

    copy_own = remote(
        o_ref, io_in.at[slot], io_send.at[0], io_recv.at[1], (image, chip * 2 + 1 - core)
    )

    @pl.loop(1, images)
    def _(step):
        copy_io(step).start()

    copy_own.start()

    for number in range(-(-p.model // LANES)):
        lanes = slice(number * LANES, (number + 1) * LANES)
        dq_s[:, 0:rows] = jnp.zeros((LANES, rows), F32) + og_ref[:, lanes].astype(F32).T
        turned = dq_s[:, 0:rows]
        for device in range(peers):
            low = max(number * LANES, device * p.share)
            high = min((number + 1) * LANES, (device + 1) * p.share)
            if low < high:
                ogt_s[device % 2, device // 2, low - device * p.share : high - device * p.share, :] = turned[
                    low - number * LANES : high - number * LANES
                ].astype(BF)

    def copy_og(step, side):
        other = (image + step) % images
        return remote(
            ogt_s.at[side, :, pl.ds(p.part_start(other), p.part)],
            og_in.at[:, :, pl.ds(pl.multiple_of(slot * rows, rows), rows)],
            og_send.at[0],
            og_recv.at[0],
            (other, chip * 2 + side),
        )

    @pl.loop(1, images)
    def _(step):
        for side in range(2):
            copy_og(step, side).start()

    for side in range(2):
        @pl.when(core != side)
        def _():
            copy_og(0, side).start()

    og_in[:, :, pl.ds(pl.multiple_of(slot * rows, rows), rows)] = ogt_s[
        core, :, pl.ds(p.part_start(image), p.part)
    ]
    io_in[slot] = o_ref[...]

    loads["w"].wait()

    @pl.loop(0, p.feature // 256)
    def _(step):
        lanes = pl.ds(pl.multiple_of(step * 256, 256), 256)
        g_cols = jnp.dot(og_ref[...], w_s[:, lanes], preferred_element_type=F32).astype(BF)
        per = 256 // width
        for number in range(per):
            head = step * per + number
            x_out[head, 1, :, 0:width] = g_cols[:, number * width : (number + 1) * width]

    pick_rows = up(p.heads, 8)
    tag = lax.broadcasted_iota(jnp.int32, (pick_rows, p.feature), 0)
    lane_at = lax.broadcasted_iota(jnp.int32, (pick_rows, p.feature), 1)
    picker = jnp.where((lane_at >= tag * width) & (lane_at < (tag + 1) * width), 1.0, 0.0).astype(F32)

    def row_dots(grads, outputs):
        product = grads.astype(F32) * outputs.astype(F32)
        return lax.dot_general(
            picker, product, NT, precision=lax.Precision.HIGHEST, preferred_element_type=F32
        )

    gathered = jnp.concatenate([x_out[head, 1, :, 0:width] for head in range(p.heads)], axis=1)
    dots_s[...] = row_dots(gathered, o_ref[...])
    loads["v"].wait()
    loads["ls"].wait()
    for head in range(p.heads):
        x_out[head, 1, :, width:depth] = v_ref[:, head * width : (head + 1) * width]
    st_out[...] = jnp.zeros_like(st_out)
    for device in range(peers):
        for j in range(p.first(device + 1) - p.first(device)):
            head = p.first(device) + j
            st_out[device, 2 * j : 2 * j + 1, :] = -ls_ref[head]
            st_out[device, 2 * j + 1 : 2 * j + 2, :] = -dots_s[head : head + 1, :]

    @pl.loop(0, peers)
    def _(step):
        device = (me + peers // 2 + step) % peers

        @pl.when(device != me)
        def _():
            copy_st(device).start()

    targets(0, lambda device, head: copy_x(0, 1)(device, head).start())
    for j in range(1, p.most):
        targets(j, lambda device, head: copy_x(j, 0)(device, head).start())

    loads["tls"].wait()
    wait_bytes(txt_s, local_sem.at[len(pairs)])
    tdots_s[...] = row_dots(txt_s[3], txt_s[4])
    st_text[...] = jnp.zeros_like(st_text)
    text_at = slice(p.tokens, p.tokens + p.text_rows)
    pad_at = slice(p.tokens + p.text_rows // SUB * SUB, p.total)

    @pl.loop(0, count)
    def _(j):
        head = first + j
        tile = pl.ds(pl.multiple_of(head // 2 * depth, depth), depth)
        odd = head % 2 == 1

        def text_cols(number):
            value = txt_s[number, :, tile]
            return jnp.where(odd, value[:, width:], value[:, :width])

        x_in[j, 0, my_rows] = x_out[head, 0]
        x_in[j, 1, my_rows] = x_out[head, 1]
        x_in[j, 0, pad_at] = jnp.zeros((p.total - pad_at.start, depth), BF)
        x_in[j, 1, pad_at] = jnp.zeros((p.total - pad_at.start, depth), BF)
        x_in[j, 0, text_at] = jnp.concatenate([text_cols(0) * jnp.asarray(scaling, BF), text_cols(1)], axis=1)
        x_in[j, 1, text_at] = jnp.concatenate([text_cols(3), text_cols(2)], axis=1)
        st_text[pl.ds(2 * j, 1), 0 : p.text_rows] = -tls_ref[head]
        st_text[pl.ds(2 * j + 1, 1), 0 : p.text_rows] = -tdots_s[pl.ds(head, 1), :]

    def stats_tile(value):
        terms = []
        for _ in range(3):
            term = value.astype(BF).astype(F32)
            terms.append(term)
            value = value - term
        used = width + 3 * p.stat_rows
        return jnp.concatenate(
            [jnp.zeros((width, LANES), F32), *terms, jnp.zeros((depth - used, LANES), F32)], axis=0
        ).T.astype(BF)

    for number in range((p.total - p.tokens) // LANES):
        stat_s[p.tokens + number * LANES : p.tokens + (number + 1) * LANES, :] = stats_tile(
            st_text[:, number * LANES : (number + 1) * LANES]
        )

    st_in[me] = st_out[me]

    wait_bytes(st_in.at[pl.ds(0, peers - 1)], st_recv.at[0])

    @pl.loop(0, peers)
    def _(source):
        stat_s[pl.ds(pl.multiple_of(source * rows, rows), rows), :] = stats_tile(st_in[source])

    lane = lax.broadcasted_iota(jnp.int32, (p.total, depth), 1)

    def ones(start):
        inside = (lane == width + start)
        for number in range(1, 3):
            inside = inside | (lane == width + start + number * p.stat_rows)
        return jnp.where(inside, 1.0, 0.0).astype(BF)[:, width:]

    far = pl.ds(0, (peers - 1) * rows)

    others = chips * p.most

    def text_slot(head, owner):
        return owner // 2 * p.most + head - p.first(owner)

    def send_text(source, head, owner, upward, downward):
        def send(way, recv, device):
            remote(source, tback_ref.at[head], text_send.at[way], text_recv.at[recv], (image, device)).start()

        @pl.when(upward & (chip + 1 < chips))
        def _():
            send(0, text_slot(head, owner), me + 2)

        @pl.when(downward & (chip > 0))
        def _():
            send(1, text_slot(head, owner), me - 2)

        send(2, others, chip * 2 + 1 - core)

    def own_back(j):
        return pltpu.make_async_copy(result_s.at[j, me], back_ref.at[first + j], own_sem.at[0])

    def ordered(head, value):
        return jnp.where(head % 2 == 1, jnp.concatenate([value[:, width:], value[:, :width]], axis=1), value)

    def send_back(j):
        own_back(j).start()

        @pl.loop(0, peers)
        def _(step):
            block = (me + peers // 2 + step) % peers

            @pl.when(block != me)
            def _():
                remote(
                    result_s.at[j, block], back_ref.at[first + j], back_send.at[0], back_recv.at[0],
                    (image, block),
                ).start()

    def own_text(j):
        return pltpu.make_async_copy(text_s.at[j], tback_ref.at[first + j], own_sem.at[1])

    half_chips = chips // 2
    side, seat = chip // half_chips, chip % half_chips
    gate = half_chips - 1 + side
    near, beyond = side * half_chips, (1 - side) * half_chips
    edge = chip != gate

    def send_sum(number, target, recv, device):
        remote(
            sums_out.at[number], target, sums_send.at[0], recv, (image, device * 2 + core)
        ).start()

    def send_terms():
        for number in range(half_chips):
            @pl.when(edge)
            def _():
                send_sum(beyond + number, gate_in.at[seat, number], gate_recv.at[0], gate)

        for number in range(half_chips):
            @pl.when(number != seat)
            def _():
                send_sum(near + number, sums_in.at[seat], sums_recv.at[0], near + number)

    def pass_sums():
        @pl.when(chip == gate)
        def _():
            if half_chips > 1:
                wait_bytes(gate_in.at[pl.ds(0, half_chips - 1)], gate_recv.at[0])
            for number in range(half_chips):
                @pl.loop(1, half_chips)
                def _(step):
                    source = (seat + step) % half_chips

                    @pl.loop(0, p.feature // 256)
                    def _(step):
                        lanes = pl.ds(pl.multiple_of(step * 256, 256), 256)
                        total = sums_out[beyond + number, :, lanes].astype(F32)
                        total += gate_in[source, number, :, lanes].astype(F32)
                        sums_out[beyond + number, :, lanes] = total.astype(BF)

                send_sum(beyond + number, sums_in.at[half_chips], sums_recv.at[0], beyond + number)

    def pass_text(hop, low, high, inward=(True, False)):
        for upward in (True, False):
            source = chip - hop if upward else chip + hop
            inner = side == (0 if upward else 1)
            wanted = {(True,): inner, (False,): ~inner}.get(inward, True)

            @pl.when((source >= 0) & (source < chips) & wanted)
            def _():
                owner = source * 2 + core
                start, stop = p.first(owner), p.first(owner + 1)

                @pl.loop(start + low, jnp.minimum(stop, start + high))
                def _(head):
                    wait_bytes(tback_ref.at[head], text_recv.at[text_slot(head, owner)])
                    send_text(tback_ref.at[head], head, owner, upward, not upward)

    @pl.loop(0, count)
    def _(j):
        head = first + j
        @pl.when(j == 0)
        def _():
            for part in range(2):
                wait_bytes(x_in.at[0, part, far], x_recv.at[part])

        @pl.when(j > 0)
        def _():
            wait_bytes(x_in.at[j, :, far], x_recv.at[1 + j])

        both = x_in[j, 0]
        q_s[...] = jnp.where(lane < width, both, stat_s[...])
        k_s[...] = jnp.concatenate([both[:, width:], ones(2 * j)], axis=1)
        both = x_in[j, 1]
        g_s[...] = jnp.where(lane < width, both, stat_s[...])
        v_s[...] = jnp.concatenate([both[:, width:], ones(2 * j + 1)], axis=1)
        dq_s[...] = jnp.zeros_like(dq_s)

        @pl.loop(0, p.total // p.key_block)
        def _(step):
            at = pl.ds(pl.multiple_of(step * p.key_block, p.key_block), p.key_block)
            keys = k_s[at, :]
            scores = lax.dot_general(keys, q_s[...], NT, preferred_element_type=F32)
            weights = jnp.exp(scores)
            grads = lax.dot_general(v_s[at, :], g_s[...], NT, preferred_element_type=F32)
            low = (weights * grads).astype(BF)
            dv_s[at, :] = jnp.dot(weights.astype(BF), g_s[...], preferred_element_type=F32).astype(BF)
            dk_s[at, :] = jnp.dot(low, q_s[...], preferred_element_type=F32).astype(BF)
            dq_s[...] += lax.dot_general(keys, low, TN, preferred_element_type=F32)

        dq = (dq_s[:, p.tokens : p.total].T * scaling).astype(BF)
        even, half = p.text_even, p.text_half
        top = jnp.concatenate([dq[:even, :width], dk_s[p.tokens : p.tokens + even, :width]], axis=1)
        bottom = jnp.concatenate(
            [dv_s[p.tokens : p.tokens + half, :width], dv_s[p.tokens + half : p.tokens + 2 * half, :width]],
            axis=1,
        )
        text_s[j, 0:even] = ordered(head, top)
        text_s[j, even : even + half] = ordered(head, bottom)
        own_text(j).start()
        send_text(text_s.at[j], head, me, True, True)

        @pl.when(j == 0)
        def _():
            if images > 1:
                wait_bytes(io_in.at[pl.ds(0, images - 1)], io_recv.at[0])

            @pl.loop(1, images)
            def _(step):
                share_io(step).start()

        @pl.when(j == 0)
        def _():
            wait_bytes(io_in.at[pl.ds(0, images)], io_recv.at[1])
            wait_bytes(og_in.at[:, :, pl.ds(0, (2 * images - 1) * rows)], og_recv.at[0])

            @pl.loop(0, p.feature // 256)
            def _(step):
                lanes = pl.ds(pl.multiple_of(step * 256, 256), 256)
                for number in range(chips):
                    total = jnp.zeros((p.part, 256), F32)
                    for source in range(2 * images):
                        total += jnp.dot(
                            og_in[number, :, source * rows : (source + 1) * rows],
                            io_in[source, :, lanes],
                            preferred_element_type=F32,
                        )
                    sums_out[number, :, lanes] = total.astype(BF)

            send_terms()

        @pl.loop(0, peers)
        def _(block):
            base = pl.multiple_of(block * rows, rows)
            dq = (dq_s[:, pl.ds(base, rows)].T * scaling).astype(BF)
            top = jnp.concatenate([dq[:, :width], dk_s[pl.ds(base, rows), :width]], axis=1)
            dv = dv_s[pl.ds(base, rows), :width]
            bottom = jnp.concatenate([dv[: rows // 2], dv[rows // 2 :]], axis=1)
            result_s[j, block, 0:rows] = ordered(head, top)
            result_s[j, block, rows : p.out_rows] = ordered(head, bottom)

        @pl.when(j == 0)
        def _():
            pass_text(1, 0, 1)

        @pl.when(j == jnp.minimum(1, count - 1))
        def _():
            pass_sums()

        @pl.when(j == jnp.where(edge, jnp.minimum(1, count - 1), 0))
        def _():
            send_back(0)


    pass_text(1, 1, p.most, (True,))

    @pl.loop(1, count)
    def _(j):
        send_back(j)

    pass_text(1, 1, 2, (False,))
    if chips > 2:
        pass_text(2, 0, 1)
    pass_text(1, 2, p.most, (False,))

    wait_bytes(sums_in.at[pl.ds(0, half_chips)], sums_recv.at[0])

    @pl.loop(0, half_chips + 1)
    def _(source):
        @pl.when(source != seat)
        def _():
            @pl.loop(0, p.feature // 256)
            def _(step):
                lanes = pl.ds(pl.multiple_of(step * 256, 256), 256)
                total = sums_out[chip, :, lanes].astype(F32) + sums_in[source, :, lanes].astype(F32)
                sums_out[chip, :, lanes] = total.astype(BF)

    own_parts = pltpu.make_async_copy(sums_out.at[chip], parts_ref.at[image], own_sem.at[2])
    own_parts.start()

    def copy_parts(step):
        return remote(
            sums_out.at[chip], parts_ref.at[image], parts_send.at[0], parts_recv.at[0],
            ((image + step) % images, me),
        )

    @pl.loop(1, images)
    def _(step):
        copy_parts(step).start()

    if chips > 2:
        pass_text(2, 1, p.most)
    for hop in range(3, chips):
        pass_text(hop, 0, p.most)

    own_parts.wait()
    if images > 1:
        wait_bytes(parts_ref.at[pl.ds(0, images - 1)], parts_recv.at[0])
        wait_bytes(parts_ref.at[pl.ds(0, images - 1)], parts_send.at[0])
    wait_bytes(io_in.at[pl.ds(0, 2 * images - 1)], io_send.at[0])
    wait_bytes(og_in.at[:, :, pl.ds(0, (2 * images - 1) * rows)], og_send.at[0])
    wait_bytes(st_in.at[pl.ds(0, peers - 1)], st_send.at[0])
    if chips > 1:
        wait_bytes(sums_out.at[pl.ds(0, chips - 1)], sums_send.at[0])

    def heads_of(number, side):
        return p.first(number * 2 + side + 1) - p.first(number * 2 + side)

    for device in range(peers):
        here, at = device // 2, device % 2
        mine = heads_of(here, at)
        same = [heads_of(number, at) for number in range(chips)]
        upward = sum(same[: here + 1]) if here + 1 < chips else 0
        downward = sum(same[here:]) if here > 0 else 0
        partner = p.heads - sum(same)

        @pl.when(me == device)
        def _():
            wait_bytes(back_ref.at[pl.ds(0, mine)], own_sem.at[0])
            wait_bytes(tback_ref.at[pl.ds(0, mine)], own_sem.at[1])
            for part in range(2):
                wait_bytes(x_out.at[pl.ds(0, peers - 1), part], x_send.at[part])
            if p.heads - peers > mine - 1:
                wait_bytes(x_out.at[pl.ds(0, p.heads - peers - mine + 1)], x_send.at[2])
            wait_bytes(result_s.at[pl.ds(0, mine), pl.ds(0, peers - 1)], back_send.at[0])
            wait_bytes(back_ref.at[pl.ds(0, p.heads - mine)], back_recv.at[0])
            for way, blocks in enumerate((upward, downward, sum(same))):
                if blocks:
                    wait_bytes(tback_ref.at[pl.ds(0, blocks)], text_send.at[way])
            wait_bytes(tback_ref.at[pl.ds(0, partner)], text_recv.at[others])


def exchange(plan, *arrays):
    p = plan
    dma = pltpu.SemaphoreType.DMA
    anywhere = pl.BlockSpec(memory_space=pl.ANY)
    pick = up(p.heads, 8)
    wide = (p.total, p.depth)
    return pl.pallas_call(
        functools.partial(exchange_kernel, p),
        out_shape=(
            jax.ShapeDtypeStruct((p.heads, p.out_rows, p.depth), BF),
            jax.ShapeDtypeStruct((p.heads, p.out_text, p.depth), BF),
            jax.ShapeDtypeStruct((p.images, p.part, p.feature), BF),
        ),
        in_specs=[anywhere] * 13,
        out_specs=(anywhere,) * 3,
        scratch_shapes=[pltpu.VMEM((p.rows, p.feature), BF)] * 4
        + [
            pltpu.VMEM((p.rows, p.model), BF),
            pltpu.VMEM((p.heads, 1, p.rows), F32),
            pltpu.VMEM((p.heads, 1, p.text_rows), F32),
            pltpu.VMEM((p.most, p.out_text, p.depth), BF),
            pltpu.VMEM((p.model, p.feature), BF),
            pltpu.VMEM((5, p.text_rows, p.feature), BF),
            pltpu.VMEM((p.heads, 2, p.rows, p.depth), BF),
            pltpu.VMEM((p.peers, p.stat_rows, p.rows), F32),
            pltpu.VMEM((p.most, 2, *wide), BF),
            pltpu.VMEM((p.peers, p.stat_rows, p.rows), F32),
            pltpu.VMEM((p.stat_rows, p.total - p.tokens), F32),
            pltpu.VMEM((pick, p.rows), F32),
            pltpu.VMEM((pick, p.text_rows), F32),
            pltpu.VMEM(wide, BF),
        ]
        + [pltpu.VMEM(wide, BF)] * 6
        + [
            pltpu.VMEM((p.depth, p.total), F32),
            pltpu.VMEM((p.most, p.peers, p.out_rows, p.depth), BF),
            pltpu.VMEM((2, p.chips, p.share_pad, p.rows), BF),
            pltpu.VMEM((p.chips, p.part, 2 * p.images * p.rows), BF),
            pltpu.VMEM((2 * p.images, p.rows, p.feature), BF),
            pltpu.VMEM((p.chips, p.part, p.feature), BF),
            pltpu.VMEM((p.chips // 2 + 1, p.part, p.feature), BF),
            pltpu.VMEM((p.chips // 2, p.chips // 2, p.part, p.feature), BF),
            dma((9,)), dma((3,)),
            dma((3,)), dma((p.most + 1,)),
            dma((1,)), dma((1,)),
            dma((1,)), dma((1,)),
            dma((3,)), dma((p.chips * p.most + 1,)),
            dma((1,)), dma((2,)),
            dma((1,)), dma((1,)),
            dma((1,)), dma((1,)), dma((1,)),
            dma((1,)), dma((1,)),
        ],
        compiler_params=pltpu.CompilerParams(
            collective_id=0, has_side_effects=True, vmem_limit_bytes=44 << 20
        ),
    )(*(pltpu.with_memory_space_constraint(array, pltpu.HBM) for array in arrays))


def finish_kernel(
    plan, back_ref, tback_ref, parts_ref, dq_out, dk_out, dv_out, tdq_out, tdk_out, tdv_out, wg_out,
    dq_ref, dk_ref, dv_ref, tdq_ref, tdk_ref, tdv_ref, wg_ref, store_sem,
):
    p = plan
    width, rows, half, even = p.width, p.rows, p.text_half, p.text_even
    group = p.heads // p.finish_steps
    stores = []

    def store(source, target):
        copy = pltpu.make_async_copy(source, target, store_sem.at[len(stores)])
        copy.start()
        stores.append(copy)

    whole = [
        pltpu.make_async_copy(source, target, store_sem.at[4 + number])
        for number, (source, target) in enumerate(((tdq_ref, tdq_out), (tdk_ref, tdk_out), (tdv_ref, tdv_out)))
    ]

    for number in range(p.images):
        start = p.part_start(number)
        stop = min(start + p.part, p.share)
        wg_ref[start:stop, :] = parts_ref[number, 0 : stop - start, :].astype(F32)
    store(wg_ref, wg_out)

    def join(ref, pair, at, left):
        even_head, odd_head = ref[2 * pair, at, :], ref[2 * pair + 1, at, :]
        lower = lax.broadcasted_iota(jnp.int32, even_head.shape, 1) < width
        if left:
            return jnp.where(lower, even_head, odd_head)
        mixed = jnp.where(lower, odd_head, even_head)
        return jnp.concatenate([mixed[:, width:], mixed[:, :width]], axis=1)

    left, right = True, False
    for pair in range(p.heads // 2):
        lanes = slice(pair * p.depth, (pair + 1) * p.depth)
        dq_ref[:, lanes] = join(back_ref, pair, slice(0, rows), left)
        dk_ref[:, lanes] = join(back_ref, pair, slice(0, rows), right)
        dv_ref[0 : rows // 2, lanes] = join(back_ref, pair, slice(rows, p.out_rows), left)
        dv_ref[rows // 2 : rows, lanes] = join(back_ref, pair, slice(rows, p.out_rows), right)
    store(dq_ref, dq_out)
    store(dk_ref, dk_out)
    store(dv_ref, dv_out)
    for step in range(p.finish_steps):
        for pair in range(step * group // 2, (step + 1) * group // 2):
            lanes = slice(pair * p.depth, (pair + 1) * p.depth)
            tdq_ref[:, lanes] = join(tback_ref, pair, slice(0, p.text_rows), left)
            tdk_ref[:, lanes] = join(tback_ref, pair, slice(0, p.text_rows), right)
            tdv_ref[0:half, lanes] = join(tback_ref, pair, slice(even, even + half), left)
            tdv_ref[half : p.text_rows, lanes] = join(tback_ref, pair, slice(even, even + p.text_rows - half), right)
        lanes = slice(step * group * width, (step + 1) * group * width)
        for number, (source, target) in enumerate(((tdq_ref, tdq_out), (tdk_ref, tdk_out), (tdv_ref, tdv_out))):
            pltpu.make_async_copy(source.at[:, lanes], target.at[:, lanes], store_sem.at[4 + number]).start()
    for copy in (*stores, *whole):
        copy.wait()


def finish(plan, back, tback, parts):
    p = plan
    anywhere = pl.BlockSpec(memory_space=pl.ANY)
    token = jax.ShapeDtypeStruct((p.rows, p.feature), BF)
    text = jax.ShapeDtypeStruct((p.text_rows, p.feature), BF)
    outs = (token,) * 3 + (text,) * 3 + (jax.ShapeDtypeStruct((p.share, p.feature), F32),)
    return pl.pallas_call(
        functools.partial(finish_kernel, p),
        out_shape=outs,
        in_specs=[pl.BlockSpec(memory_space=pltpu.VMEM)] * 3,
        out_specs=(anywhere,) * 7,
        scratch_shapes=[pltpu.VMEM(value.shape, value.dtype) for value in outs]
        + [pltpu.SemaphoreType.DMA((7,))],
        compiler_params=pltpu.CompilerParams(vmem_limit_bytes=24 << 20),
    )(back, tback, parts)


def shards(
    image_query,
    image_key,
    image_value,
    image_output,
    output_grad,
    image_logsum,
    text_query,
    text_key,
    text_value,
    text_output,
    text_grad,
    text_logsum,
    out_weight,
):
    plan = Plan(
        lax.axis_size("seq"),
        lax.axis_size("img"),
        image_query.shape[1],
        text_query.shape[1],
        output_grad.shape[2],
        image_query.shape[2],
        image_logsum.shape[2],
    )
    results = exchange(
        plan,
        image_query[0], image_key[0], image_value[0], image_output[0], output_grad[0], image_logsum.transpose(2, 0, 1),
        text_query[0], text_key[0], text_value[0], text_output[0], text_grad[0], text_logsum.transpose(2, 0, 1),
        out_weight,
    )
    *grads, weight_grad = finish(plan, *results)
    return (*(grad[None] for grad in grads), weight_grad)


def solution(mesh):
    token = P("img", "seq", None)
    text = P("img", None, None)
    return jax.shard_map(
        shards,
        mesh=mesh,
        in_specs=(token,) * 6 + (text,) * 6 + (P(),),
        out_specs=(token,) * 3 + (text,) * 3 + (P("seq", None),),
        check_vma=False,
    )
```
